16 devices in a mesh: dp: 2 (over z), tp: 8 (over y, x, core).
Axes of the slice: x: 2, y: 2, z: 2, core: 2. Of those that a mesh axis runs over, the one named last changes fastest.
Arguments:
- hidden: bfloat16 [8192, 960], P('dp')
- w_final: float32 [960], replicated
- emb_table: bfloat16 [49152, 960], P('tp')
- teacher: bfloat16 [8192, 49152], P('dp', 'tp')
- tok_mask: float32 [8192], P('dp')
Outputs:
- output 1: float32 [], replicated
- output 2: bfloat16 [8192, 960], P('dp')
- output 3: float32 [960], replicated
- output 4: float32 [49152, 960], P('tp')
All inputs are finite; a program needn't handle non-finite values.
Results may differ from the reference program's by a relative error of at most 0.00108574.
Values sent between devices are 32-bit elements.
A program may use at most 1 GiB of HBM per device.

```python
import math
import jax
import jax.numpy as jnp
from jax import lax

MODEL_DIM = 960
VOCAB_SIZE = 49152
NUM_TOKENS = 8192
SEQ_LEN = 16
ROW_BLOCK = math.gcd(NUM_TOKENS, 64)
SOFT_CAP = 30.0
NORM_EPS = 1e-6


def setup_inputs(seed: int = 0) -> dict:
    root_key = jax.random.key(seed)
    k_hid, k_gain, k_dir, k_tab, k_off, k_tea, k_seq, k_tok = jax.random.split(root_key, 8)
    fan_scale = 1.0 / math.sqrt(MODEL_DIM)
    hidden = 3.0 * jax.random.normal(k_hid, (NUM_TOKENS, MODEL_DIM), jnp.float32)
    w_final = 0.3 * jax.random.normal(k_gain, (MODEL_DIM,), jnp.float32)
    direction = 15.0 * fan_scale * jax.random.normal(k_dir, (MODEL_DIM,), jnp.float32)
    emb_table = direction[None, :] + 2.0 * fan_scale * jax.random.normal(k_tab, (VOCAB_SIZE, MODEL_DIM), jnp.float32)
    offset = 15.0 * jax.random.normal(k_off, (NUM_TOKENS, 1), jnp.float32)
    teacher = offset + 3.0 * jax.random.normal(k_tea, (NUM_TOKENS, VOCAB_SIZE), jnp.float32)
    seq_keep = (jax.random.randint(k_seq, (NUM_TOKENS // SEQ_LEN,), 0, 4) > 0).at[0].set(True)
    tok_keep = (jax.random.randint(k_tok, (NUM_TOKENS,), 0, 8) > 0).at[0].set(True)
    tok_mask = jnp.logical_and(jnp.repeat(seq_keep, SEQ_LEN), tok_keep).astype(jnp.float32)
    return {'hidden': hidden.astype(jnp.bfloat16), 'w_final': w_final, 'emb_table': emb_table.astype(jnp.bfloat16), 'teacher': teacher.astype(jnp.bfloat16), 'tok_mask': tok_mask}


def final_norm(hid_rows, w_final):
    hid_f = hid_rows.astype(jnp.float32)
    inv_rms = lax.rsqrt(jnp.mean(hid_f * hid_f, axis=-1, keepdims=True) + NORM_EPS)
    normed = hid_f * inv_rms
    return inv_rms, normed, (normed * (1.0 + w_final)).astype(jnp.bfloat16)


def reference(hidden, w_final, emb_table, teacher, tok_mask):
    mask_sum = jnp.sum(tok_mask)
    num_blocks = NUM_TOKENS // ROW_BLOCK
    hid_blocks = hidden.reshape(num_blocks, ROW_BLOCK, MODEL_DIM)
    tea_blocks = teacher.reshape(num_blocks, ROW_BLOCK, VOCAB_SIZE)
    mask_blocks = tok_mask.reshape(num_blocks, ROW_BLOCK)

    def block_step(scan_carry, block_in):
        loss_acc, gain_acc, table_acc = scan_carry
        hid_rows, tea_rows, mask_rows = block_in
        inv_rms, normed, x_rows = final_norm(hid_rows, w_final)
        logits = jnp.dot(x_rows, emb_table.T, preferred_element_type=jnp.float32)
        stu_cap = SOFT_CAP * jnp.tanh(logits / SOFT_CAP)
        tea_cap = SOFT_CAP * jnp.tanh(tea_rows.astype(jnp.float32) / SOFT_CAP)
        stu_logp = stu_cap - jax.nn.logsumexp(stu_cap, axis=-1, keepdims=True)
        tea_logp = tea_cap - jax.nn.logsumexp(tea_cap, axis=-1, keepdims=True)
        tea_prob = jnp.exp(tea_logp)
        kl_rows = jnp.sum(tea_prob * (tea_logp - stu_logp), axis=-1)
        weight = (mask_rows / mask_sum)[:, None]
        cap_ratio = stu_cap / SOFT_CAP
        grad_z = ((jnp.exp(stu_logp) - tea_prob) * weight * (1.0 - cap_ratio * cap_ratio)).astype(jnp.bfloat16)
        grad_x = jnp.dot(grad_z, emb_table, preferred_element_type=jnp.float32)
        grad_n = grad_x * (1.0 + w_final)
        grad_h = inv_rms * (grad_n - normed * jnp.mean(grad_n * normed, axis=-1, keepdims=True))
        loss_acc = loss_acc + jnp.sum(mask_rows * kl_rows)
        gain_acc = gain_acc + jnp.sum(grad_x * normed, axis=0)
        table_acc = table_acc + jnp.dot(grad_z.T, x_rows, preferred_element_type=jnp.float32)
        return (loss_acc, gain_acc, table_acc), grad_h.astype(jnp.bfloat16)

    init_carry = (jnp.zeros((), jnp.float32), jnp.zeros((MODEL_DIM,), jnp.float32), jnp.zeros((VOCAB_SIZE, MODEL_DIM), jnp.float32))
    (loss_acc, gain_acc, table_acc), grad_blocks = lax.scan(block_step, init_carry, (hid_blocks, tea_blocks, mask_blocks))
    return loss_acc / mask_sum, grad_blocks.reshape(NUM_TOKENS, MODEL_DIM), gain_acc, table_acc
```

```python
import functools

import jax
import jax.numpy as jnp
from jax import lax
from jax.experimental import pallas as pl
from jax.experimental.pallas import tpu as pltpu
from jax.sharding import PartitionSpec as P


SOFT_CAP = 30.0
NORM_EPS = 1e-6
INV_CAP = 1.0 / SOFT_CAP
EXP_SCALE = SOFT_CAP * 1.4426950408889634
TOK = 512
LINES = TOK // 128
RUN = 16
STOK = 256
COL = 512
BACK = 512
GCOL = 256
CHUNKS = (256, 256, 512, 1024, 2048, 1536, 256, 256)
VMEM_LIMIT = 62 * 1024 * 1024
MESH = pl.DeviceIdType.MESH
NT = (((1,), (1,)), ((), ()))
NN = (((1,), (0,)), ((), ()))


def stats_kernel(mask_ref, gain_ref, hid_hbm, tab_hbm, tea_hbm, x_hbm, xt_hbm, out_ref,
                 hid_buf, x_buf, xt_buf, tab_buf, tea_buf, rows_ref, z0_ref, z1_ref, acc_ref, sum_ref, gain_buf, flag_buf,
                 flags, order, hid_sem, tab_sem, tea_sem, flag_sem, out_sem):
    z_refs = (z0_ref, z1_ref)
    dim, tokens = hid_hbm.shape
    count = tab_hbm.shape[1] // COL
    slabs = tokens // TOK
    runs = tokens // RUN
    per = STOK // RUN

    def hid_copy(i):
        cols = pl.ds(i * TOK, TOK)
        return pltpu.make_async_copy(hid_hbm.at[:, cols], hid_buf.at[:, cols], hid_sem.at[i])

    def tab_copy(i):
        cols = pl.ds(i * COL, COL)
        return pltpu.make_async_copy(tab_hbm.at[:, cols], tab_buf.at[:, cols], tab_sem)

    for i in range(slabs):
        hid_copy(i).start()
    for i in range(count):
        tab_copy(i).start()

    flag = mask_ref[...]
    for shift in (1, 2, 4, 8):
        flag = jnp.maximum(flag, pltpu.roll(flag, 128 - shift, 1))
    flag_buf[...] = (flag > 0).astype(jnp.int32)
    flag_copy = pltpu.make_async_copy(flag_buf, flags, flag_sem)
    flag_copy.start()
    gain_buf[...] = jnp.broadcast_to(1.0 + gain_ref[...], (128, dim)).T
    sum_ref[...] = jnp.ones_like(sum_ref)
    flag_copy.wait()

    def mark(r, found):
        order[found] = r
        return found + flags[lax.div(r, 128 // RUN), lax.rem(r, 128 // RUN) * RUN]

    found = lax.fori_loop(0, runs, mark, 0)
    last = order[jnp.maximum(found - 1, 0)]
    last = jnp.where(found > 0, last, 0)

    def fill(k, _):
        order[found + k] = last
        return 0

    lax.fori_loop(0, 2 * per, fill, 0)
    blocks = lax.div(found + per - 1, per)

    def tea_start(b):
        slot = lax.rem(b, 2)

        def one(k, _):
            src = pl.ds(pl.multiple_of(order[b * per + k] * RUN, RUN), RUN)
            dst = pl.ds(pl.multiple_of(k * RUN, RUN), RUN)
            pltpu.make_async_copy(tea_hbm.at[src, :], tea_buf.at[slot, dst, :], tea_sem.at[slot]).start()
            return 0

        lax.fori_loop(0, per, one, 0)

    def tea_wait(b):
        slot = lax.rem(b, 2)
        pltpu.make_async_copy(tea_hbm.at[pl.ds(0, STOK), :], tea_buf.at[slot], tea_sem.at[slot]).wait()

    @pl.when(blocks > 0)
    def _():
        tea_start(0)

    def slab(i, _):
        pltpu.make_async_copy(hid_hbm.at[:, pl.ds(0, TOK)], hid_buf.at[:, pl.ds(0, TOK)], hid_sem.at[i]).wait()
        for b in range(LINES):
            lanes = pl.ds(pl.multiple_of(i * TOK + b * 128, 128), 128)
            hid = hid_buf[:, lanes].astype(jnp.float32)
            inv_rms = lax.rsqrt(jnp.mean(hid * hid, axis=0, keepdims=True) + NORM_EPS)
            xb = (hid * inv_rms * gain_buf[...]).astype(jnp.bfloat16)
            xt_buf[:, lanes] = xb
            x_buf[lanes, :] = xb.T
        return 0

    lax.fori_loop(0, slabs, slab, 0)
    x_out = pltpu.make_async_copy(x_buf, x_hbm, out_sem.at[0])
    xt_out = pltpu.make_async_copy(xt_buf, xt_hbm, out_sem.at[1])
    x_out.start()
    xt_out.start()
    pltpu.make_async_copy(tab_hbm, tab_buf, tab_sem).wait()

    def gather(b):
        slot = lax.rem(b, 2)
        for k in range(per):
            src = pl.ds(pl.multiple_of(order[b * per + k] * RUN, RUN), RUN)
            rows_ref[slot, k * RUN:(k + 1) * RUN, :] = x_buf[src, :]

    def logits(b, n, par):
        cols = slice(n * COL, (n + 1) * COL)
        z_refs[par][...] = lax.dot_general(rows_ref[lax.rem(b, 2)], tab_buf[:, cols], NN, preferred_element_type=jnp.float32)

    def collect(b, n, par):
        slot = lax.rem(b, 2)
        for r in range(0, STOK, 64):
            rows = slice(r, r + 64)
            acc_s = jnp.zeros((64, 128), jnp.float32) if n == 0 else acc_ref[0, rows, :]
            acc_t = jnp.zeros((64, 128), jnp.float32) if n == 0 else acc_ref[1, rows, :]
            for q in range(COL // 128):
                zq = z_refs[par][rows, q * 128:(q + 1) * 128]
                tq = tea_buf[slot, rows, n * COL + q * 128:n * COL + (q + 1) * 128].astype(jnp.float32)
                acc_s += jnp.exp2(jnp.tanh(zq * INV_CAP) * EXP_SCALE)
                acc_t += jnp.exp2(jnp.tanh(tq * INV_CAP) * EXP_SCALE)
            acc_ref[0, rows, :] = acc_s
            acc_ref[1, rows, :] = acc_t

    @pl.when(blocks > 0)
    def _():
        gather(0)
        logits(0, 0, 0)

    def block(b, _):
        @pl.when(b + 1 < blocks)
        def _():
            tea_start(b + 1)

        tea_wait(b)
        gather(b + 1)
        for n in range(count):
            if n + 1 < count:
                logits(b, n + 1, (n + 1) % 2)
            else:
                logits(b + 1, 0, 0)
            collect(b, n, n % 2)
        for k in range(per):
            dst = pl.ds(pl.multiple_of(order[b * per + k] * RUN, RUN), RUN)
            for s in range(2):
                sum_ref[s, dst, :] = acc_ref[s, k * RUN:(k + 1) * RUN, :]
        return 0

    lax.fori_loop(0, blocks, block, 0)

    def lines(i, _):
        for s in range(2):
            for b in range(8):
                rows = pl.ds(pl.multiple_of((i * 8 + b) * 128, 128), 128)
                out_ref[s * (tokens // 128) + i * 8 + b, :] = jnp.sum(sum_ref[s, rows, :].T, axis=0)
        return 0

    lax.fori_loop(0, tokens // 1024, lines, 0)
    x_out.wait()
    xt_out.wait()


def stats_call(mask_lines, gain_row, hid_t, tab_t, tea_rows):
    dim, tokens = hid_t.shape
    cols = tab_t.shape[1]
    assert (cols // COL) % 2 == 0
    hbm = pl.BlockSpec(memory_space=pl.ANY)
    vmem = pl.BlockSpec(memory_space=pltpu.VMEM)
    per = STOK // RUN
    return pl.pallas_call(
        stats_kernel,
        in_specs=[vmem, vmem, hbm, hbm, hbm],
        out_specs=[hbm, hbm, vmem],
        out_shape=[
            jax.ShapeDtypeStruct((tokens, dim), jnp.bfloat16),
            jax.ShapeDtypeStruct((dim, tokens), jnp.bfloat16),
            jax.ShapeDtypeStruct((tokens // 64, 128), jnp.float32),
        ],
        scratch_shapes=[
            pltpu.VMEM((dim, tokens), jnp.bfloat16),
            pltpu.VMEM((tokens, dim), jnp.bfloat16),
            pltpu.VMEM((dim, tokens), jnp.bfloat16),
            pltpu.VMEM((dim, cols), jnp.bfloat16),
            pltpu.VMEM((2, STOK, cols), jnp.bfloat16),
            pltpu.VMEM((2, STOK, dim), jnp.bfloat16),
            pltpu.VMEM((STOK, COL), jnp.float32),
            pltpu.VMEM((STOK, COL), jnp.float32),
            pltpu.VMEM((2, STOK, 128), jnp.float32),
            pltpu.VMEM((2, tokens, 128), jnp.float32),
            pltpu.VMEM((dim, 128), jnp.float32),
            pltpu.VMEM((tokens // 128, 128), jnp.int32),
            pltpu.SMEM((tokens // 128, 128), jnp.int32),
            pltpu.SMEM((tokens // RUN + 2 * per,), jnp.int32),
            pltpu.SemaphoreType.DMA((tokens // TOK,)),
            pltpu.SemaphoreType.DMA,
            pltpu.SemaphoreType.DMA((2,)),
            pltpu.SemaphoreType.DMA,
            pltpu.SemaphoreType.DMA((2,)),
        ],
        compiler_params=pltpu.CompilerParams(vmem_limit_bytes=VMEM_LIMIT),
        cost_estimate=pl.CostEstimate(flops=2 * tokens * cols * dim, bytes_accessed=2 * tokens * cols, transcendentals=0),
        name="stats",
    )(mask_lines, gain_row, hid_t, tab_t, tea_rows)


def exchange_kernel(tp, stats_ref, mask_ref, ab_ref, log_ref, slots, mask_slot, send_sem, recv_sem, msend_sem, mrecv_sem):
    dp_me = lax.axis_index("dp")
    me = lax.axis_index("tp")
    barrier = pltpu.get_barrier_semaphore()
    for d in range(1, tp):
        pl.semaphore_signal(barrier, inc=1, device_id=(dp_me, lax.rem(me + d, tp)), device_id_type=MESH)
    pl.semaphore_signal(barrier, inc=1, device_id=(1 - dp_me, me), device_id_type=MESH)
    pl.semaphore_wait(barrier, tp)

    copies = []
    for d in range(1, tp):
        copies.append(pltpu.make_async_remote_copy(
            src_ref=stats_ref, dst_ref=slots.at[me], send_sem=send_sem.at[d], recv_sem=recv_sem.at[d],
            device_id=(dp_me, lax.rem(me + d, tp)), device_id_type=MESH))
    copies.append(pltpu.make_async_remote_copy(
        src_ref=mask_ref, dst_ref=mask_slot, send_sem=msend_sem, recv_sem=mrecv_sem,
        device_id=(1 - dp_me, me), device_id_type=MESH))
    for copy in copies:
        copy.start()
    slots[me] = stats_ref[...]
    for copy in copies:
        copy.wait()
    total = slots[0]
    for k in range(1, tp):
        total += slots[k]
    mask = mask_ref[...]
    weight = mask / (jnp.sum(mask, keepdims=True) + jnp.sum(mask_slot[...], keepdims=True))
    half = mask.shape[0]
    ab_ref[:half, :] = weight / total[:half]
    ab_ref[half:, :] = weight / total[half:]
    logs = weight * (jnp.log(total[:half]) - jnp.log(total[half:]))
    log_ref[...] = jnp.sum(logs.reshape(-1, 8, 128), axis=0)


def exchange_call(stats, mask_lines, tp):
    whole = pl.BlockSpec(memory_space=pltpu.VMEM)
    return pl.pallas_call(
        functools.partial(exchange_kernel, tp),
        in_specs=[whole, whole],
        out_specs=[whole, whole],
        out_shape=[jax.ShapeDtypeStruct(stats.shape, jnp.float32), jax.ShapeDtypeStruct((8, 128), jnp.float32)],
        scratch_shapes=[
            pltpu.VMEM((tp,) + stats.shape, jnp.float32),
            pltpu.VMEM(mask_lines.shape, jnp.float32),
            pltpu.SemaphoreType.DMA((tp,)),
            pltpu.SemaphoreType.DMA((tp,)),
            pltpu.SemaphoreType.DMA,
            pltpu.SemaphoreType.DMA,
        ],
        compiler_params=pltpu.CompilerParams(collective_id=0, has_side_effects=True),
        name="exchange",
    )(stats, mask_lines)


def grad_kernel(first, ab_ref, x_ref, xt_ref, tab_ref, tea_ref, *refs):
    if first:
        table_ref, g_ref, kl_ref, z0_ref, z1_ref, coef_ref = refs
    else:
        kl_in_ref, table_ref, g_ref, kl_ref, z0_ref, z1_ref, coef_ref = refs
    z_refs = (z0_ref, z1_ref)
    col = z0_ref.shape[1]
    count = tab_ref.shape[1] // col
    block = pl.program_id(0)

    @pl.when(block == 0)
    def _():
        table_ref[...] = jnp.zeros_like(table_ref)
        kl_ref[...] = jnp.zeros_like(kl_ref) if first else kl_in_ref[...]

    for k in range(2):
        for b in range(LINES):
            line = ab_ref[pl.ds(k * (ab_ref.shape[0] // 2) + block * LINES + b, 1), :]
            coef_ref[k, b * 128:(b + 1) * 128, :] = jnp.broadcast_to(line, (128, 128)).T

    def columns(n):
        return pl.ds(pl.multiple_of(n * col, col), col)

    def logits(n, par):
        z_refs[par][...] = lax.dot_general(x_ref[...], tab_ref[:, columns(n)], NN, preferred_element_type=jnp.float32)

    def weigh(n, par):
        kl_acc = kl_ref[...]
        for r in range(0, TOK, 64):
            rows = slice(r, r + 64)
            a = coef_ref[0, rows, :]
            b = coef_ref[1, rows, :]
            for q in range(col // 128):
                lanes = pl.ds(pl.multiple_of(n * col + q * 128, 128), 128)
                zq = z_refs[par][rows, q * 128:(q + 1) * 128]
                tq = tea_ref[rows, lanes].astype(jnp.float32)
                ts = jnp.tanh(zq * INV_CAP)
                tt = jnp.tanh(tq * INV_CAP)
                pa = jnp.exp2(ts * EXP_SCALE) * a
                pb = jnp.exp2(tt * EXP_SCALE) * b
                kl = pb * (tt - ts)
                for w in range(0, 64, 8):
                    kl_acc += kl[w:w + 8]
                g_ref[rows, lanes] = ((pa - pb) * (1.0 - ts * ts)).astype(jnp.bfloat16)
        kl_ref[...] = kl_acc

    def product(n):
        table_ref[:, columns(n)] += lax.dot_general(xt_ref[...], g_ref[:, columns(n)], NN, preferred_element_type=jnp.float32)

    logits(0, 0)
    if count == 1:
        weigh(0, 0)
        product(0)
        return
    logits(1, 1)
    weigh(0, 0)

    def pair(p, _):
        for par in range(2):
            n = 2 * p + par
            logits(n, par)
            weigh(n - 1, 1 - par)
            product(n - 2)
        return 0

    if count == 4:
        pair(1, 0)
    elif count > 4:
        lax.fori_loop(1, count // 2, pair, 0)
    product(count - 2)
    weigh(count - 1, 1)
    product(count - 1)


def grad_call(ab, x_rows, x_t, tab_t, tea_rows, start, size, kl):
    tokens, dim = x_rows.shape
    first = kl is None
    col = min(GCOL, size)
    assert size == col or size % (2 * col) == 0
    in_specs = [
        pl.BlockSpec(ab.shape, lambda i: (0, 0)),
        pl.BlockSpec((TOK, dim), lambda i: (i, 0)),
        pl.BlockSpec((dim, TOK), lambda i: (0, i)),
        pl.BlockSpec((pl.Element(dim), pl.Element(size)), lambda i: (0, start), pipeline_mode=pl.Buffered(1)),
        pl.BlockSpec((pl.Element(TOK), pl.Element(size)), lambda i: (i * TOK, start)),
    ]
    operands = [ab, x_rows, x_t, tab_t, tea_rows]
    if not first:
        in_specs.append(pl.BlockSpec((8, 128), lambda i: (0, 0)))
        operands.append(kl)
    return pl.pallas_call(
        functools.partial(grad_kernel, first),
        grid=(tokens // TOK,),
        in_specs=in_specs,
        out_specs=[
            pl.BlockSpec((dim, size), lambda i: (0, 0)),
            pl.BlockSpec((TOK, size), lambda i: (i, 0)),
            pl.BlockSpec((8, 128), lambda i: (0, 0)),
        ],
        out_shape=[
            jax.ShapeDtypeStruct((dim, size), jnp.float32),
            jax.ShapeDtypeStruct((tokens, size), jnp.bfloat16),
            jax.ShapeDtypeStruct((8, 128), jnp.float32),
        ],
        scratch_shapes=[
            pltpu.VMEM((TOK, col), jnp.float32),
            pltpu.VMEM((TOK, col), jnp.float32),
            pltpu.VMEM((2, TOK, 128), jnp.float32),
        ],
        compiler_params=pltpu.CompilerParams(vmem_limit_bytes=VMEM_LIMIT),
        cost_estimate=pl.CostEstimate(flops=4 * tokens * size * dim, bytes_accessed=4 * tokens * size, transcendentals=0),
    )(*operands)


def back_kernel(half_ref, tab_ref, *refs):
    g_refs, dx_ref = refs[:-1], refs[-1]
    start = 0
    for g_ref in g_refs:
        size = g_ref.shape[1]
        step = min(BACK, size)
        for n in range(size // step):
            cols = slice(start + n * step, start + (n + 1) * step)
            dx = lax.dot_general(tab_ref[:, cols], g_ref[:, n * step:(n + 1) * step], NT, preferred_element_type=jnp.float32)
            if start + n == 0:
                dx_ref[...] = dx
            else:
                dx_ref[...] += dx
        start += size


def back_call(tab_t, grads, half):
    dim, cols = tab_t.shape
    tokens = grads[0].shape[0]
    rows = dim // 2
    return pl.pallas_call(
        back_kernel,
        grid_spec=pltpu.PrefetchScalarGridSpec(
            num_scalar_prefetch=1,
            grid=(tokens // TOK,),
            in_specs=[pl.BlockSpec((rows, cols), lambda i, h: (h[0], 0), pipeline_mode=pl.Buffered(1))]
            + [pl.BlockSpec((TOK, g.shape[1]), lambda i, h: (i, 0)) for g in grads],
            out_specs=pl.BlockSpec((rows, TOK), lambda i, h: (0, i)),
        ),
        out_shape=jax.ShapeDtypeStruct((rows, tokens), jnp.float32),
        compiler_params=pltpu.CompilerParams(vmem_limit_bytes=VMEM_LIMIT),
        cost_estimate=pl.CostEstimate(flops=tokens * cols * dim, bytes_accessed=2 * tokens * cols, transcendentals=0),
        name="back",
    )(half[None], tab_t, *grads)


def finish_kernel(off_ref, hid_ref, gain_ref, *refs):
    piece_refs, (out_ref, norm_ref, a_ref, gain_buf) = refs[:-4], refs[-4:]
    dim, toks = hid_ref.shape

    @pl.when(pl.program_id(0) == 0)
    def _():
        gain_buf[...] = jnp.broadcast_to(1.0 + gain_ref[...], (128, dim)).T

    hid = hid_ref[...].astype(jnp.float32)
    inv_rms = lax.rsqrt(jnp.mean(hid * hid, axis=0, keepdims=True) + NORM_EPS)
    norm_ref[...] = hid * inv_rms
    dot = jnp.zeros((1, toks), jnp.float32)
    for k, piece_ref in enumerate(piece_refs):
        rows = pl.ds(pl.multiple_of(off_ref[k], 8), piece_ref.shape[0])
        gain = gain_buf[rows, :]
        for b in range(toks // 128):
            a_ref[rows, b * 128:(b + 1) * 128] = piece_ref[:, b * 128:(b + 1) * 128] * gain
        dot += jnp.sum(a_ref[rows, :] * norm_ref[rows, :], axis=0, keepdims=True)
    out_ref[...] = (inv_rms * (a_ref[...] - norm_ref[...] * (dot / dim))).astype(jnp.bfloat16)


def finish_call(offsets, hid_t, gain_row, pieces):
    dim, tokens = hid_t.shape
    rows = pieces[0].shape[0]
    return pl.pallas_call(
        finish_kernel,
        grid_spec=pltpu.PrefetchScalarGridSpec(
            num_scalar_prefetch=1,
            grid=(tokens // TOK,),
            in_specs=[pl.BlockSpec((dim, TOK), lambda i, o: (0, i)), pl.BlockSpec((1, dim), lambda i, o: (0, 0))]
            + [pl.BlockSpec((rows, TOK), lambda i, o: (0, i))] * len(pieces),
            out_specs=pl.BlockSpec((dim, TOK), lambda i, o: (0, i)),
            scratch_shapes=[pltpu.VMEM((dim, TOK), jnp.float32), pltpu.VMEM((dim, TOK), jnp.float32), pltpu.VMEM((dim, 128), jnp.float32)],
        ),
        out_shape=jax.ShapeDtypeStruct((dim, tokens), jnp.bfloat16),
        compiler_params=pltpu.CompilerParams(vmem_limit_bytes=VMEM_LIMIT),
        cost_estimate=pl.CostEstimate(flops=10 * tokens * dim, bytes_accessed=8 * tokens * dim, transcendentals=0),
        name="finish",
    )(offsets, hid_t, gain_row, *pieces)


def add_kernel(own_ref, recv_ref, *refs):
    refs[-1][...] = own_ref[...] + recv_ref[...]


def add_call(own, recv, start, cols, out, after):
    dim, size = own.shape
    step = 128
    spec = pl.BlockSpec((dim, step), lambda i: (0, i))
    hold = pl.BlockSpec(memory_space=pl.ANY)
    in_specs = [spec, spec]
    operands = [own, recv]
    aliases = {}
    if out is not None:
        operands.append(out)
        aliases = {2: 0}
    operands += after
    in_specs += [hold] * (len(operands) - 2)
    return pl.pallas_call(
        add_kernel,
        grid=(size // step,),
        in_specs=in_specs,
        out_specs=pl.BlockSpec((dim, step), lambda i: (0, start // step + i)),
        out_shape=jax.ShapeDtypeStruct((dim, cols), jnp.float32),
        input_output_aliases=aliases,
        cost_estimate=pl.CostEstimate(flops=size * dim, bytes_accessed=12 * size * dim, transcendentals=0),
    )(*operands)


def exchange_partner(i, step):
    if step == 0:
        return i ^ 1
    return i ^ (2 if (i & 1) == (step - 1) else 4)


def place(bits, rows):
    return (bits[0] * (rows // 2) + bits[1] * (rows // 4) + bits[2] * (rows // 8)).astype(jnp.int32)


def solution(mesh):
    tp = mesh.shape["tp"]

    def local_step(hid_rows, w_final, tab_rows, tea_rows, mask_rows):
        tokens, dim = hid_rows.shape
        hid_t, tab_t = hid_rows.T, tab_rows.T
        mask_lines = mask_rows.reshape(tokens // 128, 128)
        x_rows, x_t, stats = stats_call(mask_lines, w_final.reshape(1, dim), hid_t, tab_t, tea_rows)
        ab, log_part = exchange_call(stats, mask_lines, tp)

        swap = [(0, 1), (1, 0)]
        kl = None
        start = 0
        parts, grads = [], []
        for c, size in enumerate(CHUNKS):
            table_c, g, kl = grad_call(ab, x_rows, x_t, tab_t, tea_rows, start, size, kl)
            grads.append(g)
            recv = lax.ppermute(table_c, "dp", swap)
            parts.append((start, table_c, recv))
            start += size

        me = lax.axis_index("tp")
        core, xb, yb = me & 1, (me >> 1) & 1, (me >> 2) & 1
        bits = (core, jnp.where(core == 0, xb, yb), jnp.where(core == 0, yb, xb))
        perms = [[(i, exchange_partner(i, s)) for i in range(tp)] for s in range(3)]
        away = back_call(tab_t, grads, 1 - core)
        recv = lax.ppermute(away, "tp", perms[0])
        keep = back_call(tab_t, grads, core)
        for s in (1, 2):
            half = keep.shape[0] // 2
            gone = (1 - bits[s]) * half
            away = lax.dynamic_slice_in_dim(keep, gone, half, 0) + lax.dynamic_slice_in_dim(recv, gone, half, 0)
            away = lax.ppermute(away, "tp", perms[s])
            kept = bits[s] * half
            keep = lax.dynamic_slice_in_dim(keep, kept, half, 0) + lax.dynamic_slice_in_dim(recv, kept, half, 0)
            recv = away
        own = keep + recv
        pieces = [own]
        for s in (2, 1, 0):
            pieces += [lax.ppermute(piece, "tp", perms[s]) for piece in pieces]
        c, u, v = bits
        spots = [(c, u, v), (c, u, 1 - v), (c, 1 - u, v), (c, 1 - u, 1 - v)]
        spots += [(1 - c, v, u), (1 - c, v, 1 - u), (1 - c, 1 - v, u), (1 - c, 1 - v, 1 - u)]
        offsets = jnp.stack([place(spot, dim) for spot in spots])

        hid_g = lax.optimization_barrier(hid_t)
        hid_f = hid_g.astype(jnp.float32)
        inv_rms = lax.rsqrt(jnp.mean(hid_f * hid_f, axis=0, keepdims=True) + NORM_EPS)
        hid_own = lax.dynamic_slice_in_dim(hid_g, offsets[0], dim // 8, 0).astype(jnp.float32)
        gain_part = jnp.sum(own * (hid_own * inv_rms), axis=1)
        loss_part = SOFT_CAP * jnp.sum(kl) + jnp.sum(log_part) / tp
        small = lax.dynamic_update_slice_in_dim(jnp.zeros((1024,), jnp.float32), gain_part, offsets[0], 0)
        small = small + jnp.where(jnp.arange(1024) == dim, loss_part, 0.0)
        small = lax.psum(small, ("dp", "tp"))
        grad_h = finish_call(offsets, hid_t, w_final.reshape(1, dim), pieces)

        out = None
        for n, (begin, own, recv) in enumerate(parts):
            last = n == len(parts) - 1
            out = add_call(own, recv, begin, tab_t.shape[1], out, [grad_h, small] if last else [])
        return small[dim], grad_h.T, small[:dim], out.T

    return jax.shard_map(local_step, mesh=mesh, in_specs=(P('dp', None), P(None), P('tp', None), P('dp', 'tp'), P('dp')), out_specs=(P(), P('dp', None), P(None), P('tp', None)), check_vma=False)
```

```python
import functools

import jax
import jax.numpy as jnp
from jax import lax
from jax.experimental import pallas as pl
from jax.experimental.pallas import tpu as pltpu
from jax.sharding import PartitionSpec as P


SOFT_CAP = 30.0
NORM_EPS = 1e-6
INV_CAP = 1.0 / SOFT_CAP
EXP_SCALE = SOFT_CAP * 1.4426950408889634
TOK = 512
LINES = TOK // 128
RUN = 16
STOK = 256
COL = 512
BACK = 512
GCOL = 256
CHUNKS = (256, 256, 512, 1024, 2048, 1536, 256, 256)
VMEM_LIMIT = 62 * 1024 * 1024
MESH = pl.DeviceIdType.MESH
NT = (((1,), (1,)), ((), ()))
NN = (((1,), (0,)), ((), ()))


def stats_kernel(mask_ref, gain_ref, hid_hbm, tab_hbm, tea_hbm, x_hbm, xt_hbm, out_ref,
                 hid_buf, x_buf, xt_buf, tab_buf, tea_buf, rows_ref, z0_ref, z1_ref, acc_ref, sum_ref, gain_buf, flag_buf,
                 flags, order, hid_sem, tab_sem, tea_sem, flag_sem, out_sem):
    z_refs = (z0_ref, z1_ref)
    dim, tokens = hid_hbm.shape
    count = tab_hbm.shape[1] // COL
    slabs = tokens // TOK
    runs = tokens // RUN
    per = STOK // RUN

    def hid_copy(i):
        cols = pl.ds(i * TOK, TOK)
        return pltpu.make_async_copy(hid_hbm.at[:, cols], hid_buf.at[:, cols], hid_sem.at[i])

    def tab_copy(i):
        cols = pl.ds(i * COL, COL)
        return pltpu.make_async_copy(tab_hbm.at[:, cols], tab_buf.at[:, cols], tab_sem)

    for i in range(slabs):
        hid_copy(i).start()
    for i in range(count):
        tab_copy(i).start()

    flag = mask_ref[...]
    for shift in (1, 2, 4, 8):
        flag = jnp.maximum(flag, pltpu.roll(flag, 128 - shift, 1))
    flag_buf[...] = (flag > 0).astype(jnp.int32)
    flag_copy = pltpu.make_async_copy(flag_buf, flags, flag_sem)
    flag_copy.start()
    gain_buf[...] = jnp.broadcast_to(1.0 + gain_ref[...], (128, dim)).T
    sum_ref[...] = jnp.ones_like(sum_ref)
    flag_copy.wait()

    def mark(r, found):
        order[found] = r
        return found + flags[lax.div(r, 128 // RUN), lax.rem(r, 128 // RUN) * RUN]

    found = lax.fori_loop(0, runs, mark, 0)
    last = order[jnp.maximum(found - 1, 0)]
    last = jnp.where(found > 0, last, 0)

    def fill(k, _):
        order[found + k] = last
        return 0

    lax.fori_loop(0, 2 * per, fill, 0)
    blocks = lax.div(found + per - 1, per)

    def tea_start(b):
        slot = lax.rem(b, 2)

        def one(k, _):
            src = pl.ds(pl.multiple_of(order[b * per + k] * RUN, RUN), RUN)
            dst = pl.ds(pl.multiple_of(k * RUN, RUN), RUN)
            pltpu.make_async_copy(tea_hbm.at[src, :], tea_buf.at[slot, dst, :], tea_sem.at[slot]).start()
            return 0

        lax.fori_loop(0, per, one, 0)

    def tea_wait(b):
        slot = lax.rem(b, 2)
        pltpu.make_async_copy(tea_hbm.at[pl.ds(0, STOK), :], tea_buf.at[slot], tea_sem.at[slot]).wait()

    @pl.when(blocks > 0)
    def _():
        tea_start(0)

    def slab(i, _):
        pltpu.make_async_copy(hid_hbm.at[:, pl.ds(0, TOK)], hid_buf.at[:, pl.ds(0, TOK)], hid_sem.at[i]).wait()
        for b in range(LINES):
            lanes = pl.ds(pl.multiple_of(i * TOK + b * 128, 128), 128)
            hid = hid_buf[:, lanes].astype(jnp.float32)
            inv_rms = lax.rsqrt(jnp.mean(hid * hid, axis=0, keepdims=True) + NORM_EPS)
            xb = (hid * inv_rms * gain_buf[...]).astype(jnp.bfloat16)
            xt_buf[:, lanes] = xb
            x_buf[lanes, :] = xb.T
        return 0

    lax.fori_loop(0, slabs, slab, 0)
    x_out = pltpu.make_async_copy(x_buf, x_hbm, out_sem.at[0])
    xt_out = pltpu.make_async_copy(xt_buf, xt_hbm, out_sem.at[1])
    x_out.start()
    xt_out.start()
    pltpu.make_async_copy(tab_hbm, tab_buf, tab_sem).wait()

    def gather(b):
        slot = lax.rem(b, 2)
        for k in range(per):
            src = pl.ds(pl.multiple_of(order[b * per + k] * RUN, RUN), RUN)
            rows_ref[slot, k * RUN:(k + 1) * RUN, :] = x_buf[src, :]

    def logits(b, n, par):
        cols = slice(n * COL, (n + 1) * COL)
        z_refs[par][...] = lax.dot_general(rows_ref[lax.rem(b, 2)], tab_buf[:, cols], NN, preferred_element_type=jnp.float32)

    def collect(b, n, par):
        slot = lax.rem(b, 2)
        for r in range(0, STOK, 64):
            rows = slice(r, r + 64)
            acc_s = jnp.zeros((64, 128), jnp.float32) if n == 0 else acc_ref[0, rows, :]
            acc_t = jnp.zeros((64, 128), jnp.float32) if n == 0 else acc_ref[1, rows, :]
            for q in range(COL // 128):
                zq = z_refs[par][rows, q * 128:(q + 1) * 128]
                tq = tea_buf[slot, rows, n * COL + q * 128:n * COL + (q + 1) * 128].astype(jnp.float32)
                acc_s += jnp.exp2(jnp.tanh(zq * INV_CAP) * EXP_SCALE)
                acc_t += jnp.exp2(jnp.tanh(tq * INV_CAP) * EXP_SCALE)
            acc_ref[0, rows, :] = acc_s
            acc_ref[1, rows, :] = acc_t

    @pl.when(blocks > 0)
    def _():
        gather(0)
        logits(0, 0, 0)

    def block(b, _):
        @pl.when(b + 1 < blocks)
        def _():
            tea_start(b + 1)

        tea_wait(b)
        gather(b + 1)
        for n in range(count):
            if n + 1 < count:
                logits(b, n + 1, (n + 1) % 2)
            else:
                logits(b + 1, 0, 0)
            collect(b, n, n % 2)
        for k in range(per):
            dst = pl.ds(pl.multiple_of(order[b * per + k] * RUN, RUN), RUN)
            for s in range(2):
                sum_ref[s, dst, :] = acc_ref[s, k * RUN:(k + 1) * RUN, :]
        return 0

    lax.fori_loop(0, blocks, block, 0)

    def lines(i, _):
        for s in range(2):
            for b in range(8):
                rows = pl.ds(pl.multiple_of((i * 8 + b) * 128, 128), 128)
                out_ref[s * (tokens // 128) + i * 8 + b, :] = jnp.sum(sum_ref[s, rows, :].T, axis=0)
        return 0

    lax.fori_loop(0, tokens // 1024, lines, 0)
    x_out.wait()
    xt_out.wait()


def stats_call(mask_lines, gain_row, hid_t, tab_t, tea_rows):
    dim, tokens = hid_t.shape
    cols = tab_t.shape[1]
    assert (cols // COL) % 2 == 0
    hbm = pl.BlockSpec(memory_space=pl.ANY)
    vmem = pl.BlockSpec(memory_space=pltpu.VMEM)
    per = STOK // RUN
    return pl.pallas_call(
        stats_kernel,
        in_specs=[vmem, vmem, hbm, hbm, hbm],
        out_specs=[hbm, hbm, vmem],
        out_shape=[
            jax.ShapeDtypeStruct((tokens, dim), jnp.bfloat16),
            jax.ShapeDtypeStruct((dim, tokens), jnp.bfloat16),
            jax.ShapeDtypeStruct((tokens // 64, 128), jnp.float32),
        ],
        scratch_shapes=[
            pltpu.VMEM((dim, tokens), jnp.bfloat16),
            pltpu.VMEM((tokens, dim), jnp.bfloat16),
            pltpu.VMEM((dim, tokens), jnp.bfloat16),
            pltpu.VMEM((dim, cols), jnp.bfloat16),
            pltpu.VMEM((2, STOK, cols), jnp.bfloat16),
            pltpu.VMEM((2, STOK, dim), jnp.bfloat16),
            pltpu.VMEM((STOK, COL), jnp.float32),
            pltpu.VMEM((STOK, COL), jnp.float32),
            pltpu.VMEM((2, STOK, 128), jnp.float32),
            pltpu.VMEM((2, tokens, 128), jnp.float32),
            pltpu.VMEM((dim, 128), jnp.float32),
            pltpu.VMEM((tokens // 128, 128), jnp.int32),
            pltpu.SMEM((tokens // 128, 128), jnp.int32),
            pltpu.SMEM((tokens // RUN + 2 * per,), jnp.int32),
            pltpu.SemaphoreType.DMA((tokens // TOK,)),
            pltpu.SemaphoreType.DMA,
            pltpu.SemaphoreType.DMA((2,)),
            pltpu.SemaphoreType.DMA,
            pltpu.SemaphoreType.DMA((2,)),
        ],
        compiler_params=pltpu.CompilerParams(vmem_limit_bytes=VMEM_LIMIT),
        cost_estimate=pl.CostEstimate(flops=2 * tokens * cols * dim, bytes_accessed=2 * tokens * cols, transcendentals=0),
        name="stats",
    )(mask_lines, gain_row, hid_t, tab_t, tea_rows)


def exchange_kernel(tp, stats_ref, mask_ref, ab_ref, log_ref, slots, mask_slot, send_sem, recv_sem, msend_sem, mrecv_sem):
    dp_me = lax.axis_index("dp")
    me = lax.axis_index("tp")
    barrier = pltpu.get_barrier_semaphore()
    for d in range(1, tp):
        pl.semaphore_signal(barrier, inc=1, device_id=(dp_me, lax.rem(me + d, tp)), device_id_type=MESH)
    pl.semaphore_signal(barrier, inc=1, device_id=(1 - dp_me, me), device_id_type=MESH)
    pl.semaphore_wait(barrier, tp)

    copies = []
    for d in range(1, tp):
        copies.append(pltpu.make_async_remote_copy(
            src_ref=stats_ref, dst_ref=slots.at[me], send_sem=send_sem.at[d], recv_sem=recv_sem.at[d],
            device_id=(dp_me, lax.rem(me + d, tp)), device_id_type=MESH))
    copies.append(pltpu.make_async_remote_copy(
        src_ref=mask_ref, dst_ref=mask_slot, send_sem=msend_sem, recv_sem=mrecv_sem,
        device_id=(1 - dp_me, me), device_id_type=MESH))
    for copy in copies:
        copy.start()
    slots[me] = stats_ref[...]
    for copy in copies:
        copy.wait()
    total = slots[0]
    for k in range(1, tp):
        total += slots[k]
    mask = mask_ref[...]
    weight = mask / (jnp.sum(mask, keepdims=True) + jnp.sum(mask_slot[...], keepdims=True))
    half = mask.shape[0]
    ab_ref[:half, :] = weight / total[:half]
    ab_ref[half:, :] = weight / total[half:]
    logs = weight * (jnp.log(total[:half]) - jnp.log(total[half:]))
    log_ref[...] = jnp.sum(logs.reshape(-1, 8, 128), axis=0)


def exchange_call(stats, mask_lines, tp):
    whole = pl.BlockSpec(memory_space=pltpu.VMEM)
    return pl.pallas_call(
        functools.partial(exchange_kernel, tp),
        in_specs=[whole, whole],
        out_specs=[whole, whole],
        out_shape=[jax.ShapeDtypeStruct(stats.shape, jnp.float32), jax.ShapeDtypeStruct((8, 128), jnp.float32)],
        scratch_shapes=[
            pltpu.VMEM((tp,) + stats.shape, jnp.float32),
            pltpu.VMEM(mask_lines.shape, jnp.float32),
            pltpu.SemaphoreType.DMA((tp,)),
            pltpu.SemaphoreType.DMA((tp,)),
            pltpu.SemaphoreType.DMA,
            pltpu.SemaphoreType.DMA,
        ],
        compiler_params=pltpu.CompilerParams(collective_id=0, has_side_effects=True),
        name="exchange",
    )(stats, mask_lines)


def grad_kernel(first, ab_ref, x_ref, xt_ref, tab_ref, tea_ref, *refs):
    if first:
        table_ref, g_ref, kl_ref, z0_ref, z1_ref, coef_ref = refs
    else:
        kl_in_ref, table_ref, g_ref, kl_ref, z0_ref, z1_ref, coef_ref = refs
    z_refs = (z0_ref, z1_ref)
    col = z0_ref.shape[1]
    count = tab_ref.shape[1] // col
    block = pl.program_id(0)

    @pl.when(block == 0)
    def _():
        table_ref[...] = jnp.zeros_like(table_ref)
        kl_ref[...] = jnp.zeros_like(kl_ref) if first else kl_in_ref[...]

    for k in range(2):
        for b in range(LINES):
            line = ab_ref[pl.ds(k * (ab_ref.shape[0] // 2) + block * LINES + b, 1), :]
            coef_ref[k, b * 128:(b + 1) * 128, :] = jnp.broadcast_to(line, (128, 128)).T

    def columns(n):
        return pl.ds(pl.multiple_of(n * col, col), col)

    def logits(n, par):
        z_refs[par][...] = lax.dot_general(x_ref[...], tab_ref[:, columns(n)], NN, preferred_element_type=jnp.float32)

    def weigh(n, par):
        kl_acc = kl_ref[...]
        for r in range(0, TOK, 64):
            rows = slice(r, r + 64)
            a = coef_ref[0, rows, :]
            b = coef_ref[1, rows, :]
            for q in range(col // 128):
                lanes = pl.ds(pl.multiple_of(n * col + q * 128, 128), 128)
                zq = z_refs[par][rows, q * 128:(q + 1) * 128]
                tq = tea_ref[rows, lanes].astype(jnp.float32)
                ts = jnp.tanh(zq * INV_CAP)
                tt = jnp.tanh(tq * INV_CAP)
                pa = jnp.exp2(ts * EXP_SCALE) * a
                pb = jnp.exp2(tt * EXP_SCALE) * b
                kl = pb * (tt - ts)
                for w in range(0, 64, 8):
                    kl_acc += kl[w:w + 8]
                g_ref[rows, lanes] = ((pa - pb) * (1.0 - ts * ts)).astype(jnp.bfloat16)
        kl_ref[...] = kl_acc

    def product(n):
        table_ref[:, columns(n)] += lax.dot_general(xt_ref[...], g_ref[:, columns(n)], NN, preferred_element_type=jnp.float32)

    logits(0, 0)
    if count == 1:
        weigh(0, 0)
        product(0)
        return
    logits(1, 1)
    weigh(0, 0)

    def pair(p, _):
        for par in range(2):
            n = 2 * p + par
            logits(n, par)
            weigh(n - 1, 1 - par)
            product(n - 2)
        return 0

    if count == 4:
        pair(1, 0)
    elif count > 4:
        lax.fori_loop(1, count // 2, pair, 0)
    product(count - 2)
    weigh(count - 1, 1)
    product(count - 1)


def grad_call(ab, x_rows, x_t, tab_t, tea_rows, start, size, kl):
    tokens, dim = x_rows.shape
    first = kl is None
    col = min(GCOL, size)
    assert size == col or size % (2 * col) == 0
    in_specs = [
        pl.BlockSpec(ab.shape, lambda i: (0, 0)),
        pl.BlockSpec((TOK, dim), lambda i: (i, 0)),
        pl.BlockSpec((dim, TOK), lambda i: (0, i)),
        pl.BlockSpec((pl.Element(dim), pl.Element(size)), lambda i: (0, start), pipeline_mode=pl.Buffered(1)),
        pl.BlockSpec((pl.Element(TOK), pl.Element(size)), lambda i: (i * TOK, start)),
    ]
    operands = [ab, x_rows, x_t, tab_t, tea_rows]
    if not first:
        in_specs.append(pl.BlockSpec((8, 128), lambda i: (0, 0)))
        operands.append(kl)
    return pl.pallas_call(
        functools.partial(grad_kernel, first),
        grid=(tokens // TOK,),
        in_specs=in_specs,
        out_specs=[
            pl.BlockSpec((dim, size), lambda i: (0, 0)),
            pl.BlockSpec((TOK, size), lambda i: (i, 0)),
            pl.BlockSpec((8, 128), lambda i: (0, 0)),
        ],
        out_shape=[
            jax.ShapeDtypeStruct((dim, size), jnp.float32),
            jax.ShapeDtypeStruct((tokens, size), jnp.bfloat16),
            jax.ShapeDtypeStruct((8, 128), jnp.float32),
        ],
        scratch_shapes=[
            pltpu.VMEM((TOK, col), jnp.float32),
            pltpu.VMEM((TOK, col), jnp.float32),
            pltpu.VMEM((2, TOK, 128), jnp.float32),
        ],
        compiler_params=pltpu.CompilerParams(vmem_limit_bytes=VMEM_LIMIT),
        cost_estimate=pl.CostEstimate(flops=4 * tokens * size * dim, bytes_accessed=4 * tokens * size, transcendentals=0),
    )(*operands)


def back_kernel(half_ref, tab_ref, *refs):
    g_refs, dx_ref = refs[:-1], refs[-1]
    start = 0
    for g_ref in g_refs:
        size = g_ref.shape[1]
        step = min(BACK, size)
        for n in range(size // step):
            cols = slice(start + n * step, start + (n + 1) * step)
            dx = lax.dot_general(tab_ref[:, cols], g_ref[:, n * step:(n + 1) * step], NT, preferred_element_type=jnp.float32)
            if start + n == 0:
                dx_ref[...] = dx
            else:
                dx_ref[...] += dx
        start += size


def back_call(tab_t, grads, half):
    dim, cols = tab_t.shape
    tokens = grads[0].shape[0]
    rows = dim // 2
    return pl.pallas_call(
        back_kernel,
        grid_spec=pltpu.PrefetchScalarGridSpec(
            num_scalar_prefetch=1,
            grid=(tokens // TOK,),
            in_specs=[pl.BlockSpec((rows, cols), lambda i, h: (h[0], 0), pipeline_mode=pl.Buffered(1))]
            + [pl.BlockSpec((TOK, g.shape[1]), lambda i, h: (i, 0)) for g in grads],
            out_specs=pl.BlockSpec((rows, TOK), lambda i, h: (0, i)),
        ),
        out_shape=jax.ShapeDtypeStruct((rows, tokens), jnp.float32),
        compiler_params=pltpu.CompilerParams(vmem_limit_bytes=VMEM_LIMIT),
        cost_estimate=pl.CostEstimate(flops=tokens * cols * dim, bytes_accessed=2 * tokens * cols, transcendentals=0),
        name="back",
    )(half[None], tab_t, *grads)


def finish_kernel(off_ref, hid_ref, gain_ref, *refs):
    piece_refs, (out_ref, sum_ref, norm_ref, a_ref, gain_buf) = refs[:-5], refs[-5:]
    dim, toks = hid_ref.shape

    @pl.when(pl.program_id(0) == 0)
    def _():
        gain_buf[...] = jnp.broadcast_to(1.0 + gain_ref[...], (128, dim)).T
        sum_ref[...] = jnp.zeros_like(sum_ref)

    hid = hid_ref[...].astype(jnp.float32)
    inv_rms = lax.rsqrt(jnp.mean(hid * hid, axis=0, keepdims=True) + NORM_EPS)
    norm_ref[...] = hid * inv_rms
    dot = jnp.zeros((1, toks), jnp.float32)
    for k, piece_ref in enumerate(piece_refs):
        rows = pl.ds(pl.multiple_of(off_ref[k], 8), piece_ref.shape[0])
        gain = gain_buf[rows, :]
        acc = sum_ref[rows, :]
        for b in range(toks // 128):
            lanes = slice(b * 128, (b + 1) * 128)
            a_ref[rows, lanes] = piece_ref[:, lanes] * gain
            acc += piece_ref[:, lanes] * norm_ref[rows, lanes]
        sum_ref[rows, :] = acc
        dot += jnp.sum(a_ref[rows, :] * norm_ref[rows, :], axis=0, keepdims=True)
    out_ref[...] = (inv_rms * (a_ref[...] - norm_ref[...] * (dot / dim))).astype(jnp.bfloat16)


def finish_call(offsets, hid_t, gain_row, pieces):
    dim, tokens = hid_t.shape
    rows = pieces[0].shape[0]
    return pl.pallas_call(
        finish_kernel,
        grid_spec=pltpu.PrefetchScalarGridSpec(
            num_scalar_prefetch=1,
            grid=(tokens // TOK,),
            in_specs=[pl.BlockSpec((dim, TOK), lambda i, o: (0, i)), pl.BlockSpec((1, dim), lambda i, o: (0, 0))]
            + [pl.BlockSpec((rows, TOK), lambda i, o: (0, i))] * len(pieces),
            out_specs=[pl.BlockSpec((dim, TOK), lambda i, o: (0, i)), pl.BlockSpec((dim, 128), lambda i, o: (0, 0))],
            scratch_shapes=[pltpu.VMEM((dim, TOK), jnp.float32), pltpu.VMEM((dim, TOK), jnp.float32), pltpu.VMEM((dim, 128), jnp.float32)],
        ),
        out_shape=[jax.ShapeDtypeStruct((dim, tokens), jnp.bfloat16), jax.ShapeDtypeStruct((dim, 128), jnp.float32)],
        compiler_params=pltpu.CompilerParams(vmem_limit_bytes=VMEM_LIMIT),
        cost_estimate=pl.CostEstimate(flops=10 * tokens * dim, bytes_accessed=8 * tokens * dim, transcendentals=0),
        name="finish",
    )(offsets, hid_t, gain_row, *pieces)


def add_kernel(own_ref, recv_ref, *refs):
    refs[-1][...] = own_ref[...] + recv_ref[...]


def add_call(own, recv, start, cols, out, after):
    dim, size = own.shape
    step = 128
    spec = pl.BlockSpec((dim, step), lambda i: (0, i))
    hold = pl.BlockSpec(memory_space=pl.ANY)
    in_specs = [spec, spec]
    operands = [own, recv]
    aliases = {}
    if out is not None:
        operands.append(out)
        aliases = {2: 0}
    operands += after
    in_specs += [hold] * (len(operands) - 2)
    return pl.pallas_call(
        add_kernel,
        grid=(size // step,),
        in_specs=in_specs,
        out_specs=pl.BlockSpec((dim, step), lambda i: (0, start // step + i)),
        out_shape=jax.ShapeDtypeStruct((dim, cols), jnp.float32),
        input_output_aliases=aliases,
        cost_estimate=pl.CostEstimate(flops=size * dim, bytes_accessed=12 * size * dim, transcendentals=0),
    )(*operands)


def exchange_partner(i, step):
    if step == 0:
        return i ^ 1
    return i ^ (2 if (i & 1) == (step - 1) else 4)


def place(bits, rows):
    return (bits[0] * (rows // 2) + bits[1] * (rows // 4) + bits[2] * (rows // 8)).astype(jnp.int32)


def solution(mesh):
    tp = mesh.shape["tp"]

    def local_step(hid_rows, w_final, tab_rows, tea_rows, mask_rows):
        tokens, dim = hid_rows.shape
        hid_t, tab_t = hid_rows.T, tab_rows.T
        mask_lines = mask_rows.reshape(tokens // 128, 128)
        x_rows, x_t, stats = stats_call(mask_lines, w_final.reshape(1, dim), hid_t, tab_t, tea_rows)
        ab, log_part = exchange_call(stats, mask_lines, tp)

        swap = [(0, 1), (1, 0)]
        kl = None
        start = 0
        parts, grads = [], []
        for c, size in enumerate(CHUNKS):
            table_c, g, kl = grad_call(ab, x_rows, x_t, tab_t, tea_rows, start, size, kl)
            grads.append(g)
            recv = lax.ppermute(table_c, "dp", swap)
            parts.append((start, table_c, recv))
            start += size

        me = lax.axis_index("tp")
        core, xb, yb = me & 1, (me >> 1) & 1, (me >> 2) & 1
        bits = (core, jnp.where(core == 0, xb, yb), jnp.where(core == 0, yb, xb))
        perms = [[(i, exchange_partner(i, s)) for i in range(tp)] for s in range(3)]
        away = back_call(tab_t, grads, 1 - core)
        recv = lax.ppermute(away, "tp", perms[0])
        keep = back_call(tab_t, grads, core)
        for s in (1, 2):
            half = keep.shape[0] // 2
            gone = (1 - bits[s]) * half
            away = lax.dynamic_slice_in_dim(keep, gone, half, 0) + lax.dynamic_slice_in_dim(recv, gone, half, 0)
            away = lax.ppermute(away, "tp", perms[s])
            kept = bits[s] * half
            keep = lax.dynamic_slice_in_dim(keep, kept, half, 0) + lax.dynamic_slice_in_dim(recv, kept, half, 0)
            recv = away
        own = keep + recv
        pieces = [own]
        for s in (2, 1, 0):
            pieces += [lax.ppermute(piece, "tp", perms[s]) for piece in pieces]
        c, u, v = bits
        spots = [(c, u, v), (c, u, 1 - v), (c, 1 - u, v), (c, 1 - u, 1 - v)]
        spots += [(1 - c, v, u), (1 - c, v, 1 - u), (1 - c, 1 - v, u), (1 - c, 1 - v, 1 - u)]
        offsets = jnp.stack([place(spot, dim) for spot in spots])

        loss_part = lax.psum(SOFT_CAP * jnp.sum(kl), "tp") + jnp.sum(log_part)
        grad_h, gain_part = finish_call(offsets, hid_t, w_final.reshape(1, dim), pieces)
        small = jnp.concatenate([jnp.sum(gain_part, axis=1), jnp.full((1024 - dim,), loss_part)])
        other = lax.ppermute(small, "dp", swap)
        small = small + other

        out = None
        for n, (begin, own, recv) in enumerate(parts):
            last = n == len(parts) - 1
            out = add_call(own, recv, begin, tab_t.shape[1], out, [grad_h, small] if last else [])
        return small[dim], grad_h.T, small[:dim], out.T

    return jax.shard_map(local_step, mesh=mesh, in_specs=(P('dp', None), P(None), P('tp', None), P('dp', 'tp'), P('dp')), out_specs=(P(), P('dp', None), P(None), P('tp', None)), check_vma=False)
```

```python
import functools

import jax
import jax.numpy as jnp
from jax import lax
from jax.experimental import pallas as pl
from jax.experimental.pallas import tpu as pltpu
from jax.sharding import PartitionSpec as P


SOFT_CAP = 30.0
NORM_EPS = 1e-6
INV_CAP = 1.0 / SOFT_CAP
EXP_SCALE = SOFT_CAP * 1.4426950408889634
TOK = 512
LINES = TOK // 128
RUN = 16
STOK = 256
COL = 512
BACK = 512
GCOL = 256
CHUNKS = (256, 256, 512, 1024, 2048, 1536, 256, 256)
VMEM_LIMIT = 62 * 1024 * 1024
MESH = pl.DeviceIdType.MESH
NT = (((1,), (1,)), ((), ()))
NN = (((1,), (0,)), ((), ()))


def stats_kernel(mask_ref, gain_ref, hid_hbm, tab_hbm, tea_hbm, x_hbm, xt_hbm, out_ref,
                 hid_buf, x_buf, xt_buf, tab_buf, tea_buf, rows_ref, z0_ref, z1_ref, acc_ref, sum_ref, gain_buf, flag_buf,
                 flags, order, hid_sem, tab_sem, tea_sem, flag_sem, out_sem):
    z_refs = (z0_ref, z1_ref)
    dim, tokens = hid_hbm.shape
    count = tab_hbm.shape[1] // COL
    slabs = tokens // TOK
    runs = tokens // RUN
    per = STOK // RUN

    def hid_copy(i):
        cols = pl.ds(i * TOK, TOK)
        return pltpu.make_async_copy(hid_hbm.at[:, cols], hid_buf.at[:, cols], hid_sem.at[i])

    def tab_copy(i):
        cols = pl.ds(i * COL, COL)
        return pltpu.make_async_copy(tab_hbm.at[:, cols], tab_buf.at[:, cols], tab_sem)

    for i in range(slabs):
        hid_copy(i).start()
    for i in range(count):
        tab_copy(i).start()

    flag = mask_ref[...]
    for shift in (1, 2, 4, 8):
        flag = jnp.maximum(flag, pltpu.roll(flag, 128 - shift, 1))
    flag_buf[...] = (flag > 0).astype(jnp.int32)
    flag_copy = pltpu.make_async_copy(flag_buf, flags, flag_sem)
    flag_copy.start()
    gain_buf[...] = jnp.broadcast_to(1.0 + gain_ref[...], (128, dim)).T
    sum_ref[...] = jnp.ones_like(sum_ref)
    flag_copy.wait()

    def mark(r, found):
        order[found] = r
        return found + flags[lax.div(r, 128 // RUN), lax.rem(r, 128 // RUN) * RUN]

    found = lax.fori_loop(0, runs, mark, 0)
    last = order[jnp.maximum(found - 1, 0)]
    last = jnp.where(found > 0, last, 0)

    def fill(k, _):
        order[found + k] = last
        return 0

    lax.fori_loop(0, 2 * per, fill, 0)
    blocks = lax.div(found + per - 1, per)

    def tea_start(b):
        slot = lax.rem(b, 2)

        def one(k, _):
            src = pl.ds(pl.multiple_of(order[b * per + k] * RUN, RUN), RUN)
            dst = pl.ds(pl.multiple_of(k * RUN, RUN), RUN)
            pltpu.make_async_copy(tea_hbm.at[src, :], tea_buf.at[slot, dst, :], tea_sem.at[slot]).start()
            return 0

        lax.fori_loop(0, per, one, 0)

    def tea_wait(b):
        slot = lax.rem(b, 2)
        pltpu.make_async_copy(tea_hbm.at[pl.ds(0, STOK), :], tea_buf.at[slot], tea_sem.at[slot]).wait()

    @pl.when(blocks > 0)
    def _():
        tea_start(0)

    def slab(i, _):
        pltpu.make_async_copy(hid_hbm.at[:, pl.ds(0, TOK)], hid_buf.at[:, pl.ds(0, TOK)], hid_sem.at[i]).wait()
        for b in range(LINES):
            lanes = pl.ds(pl.multiple_of(i * TOK + b * 128, 128), 128)
            hid = hid_buf[:, lanes].astype(jnp.float32)
            inv_rms = lax.rsqrt(jnp.mean(hid * hid, axis=0, keepdims=True) + NORM_EPS)
            xb = (hid * inv_rms * gain_buf[...]).astype(jnp.bfloat16)
            xt_buf[:, lanes] = xb
            x_buf[lanes, :] = xb.T
        return 0

    lax.fori_loop(0, slabs, slab, 0)
    x_out = pltpu.make_async_copy(x_buf, x_hbm, out_sem.at[0])
    xt_out = pltpu.make_async_copy(xt_buf, xt_hbm, out_sem.at[1])
    x_out.start()
    xt_out.start()
    pltpu.make_async_copy(tab_hbm, tab_buf, tab_sem).wait()

    def gather(b):
        slot = lax.rem(b, 2)
        for k in range(per):
            src = pl.ds(pl.multiple_of(order[b * per + k] * RUN, RUN), RUN)
            rows_ref[slot, k * RUN:(k + 1) * RUN, :] = x_buf[src, :]

    def logits(b, n, par):
        cols = slice(n * COL, (n + 1) * COL)
        z_refs[par][...] = lax.dot_general(rows_ref[lax.rem(b, 2)], tab_buf[:, cols], NN, preferred_element_type=jnp.float32)

    def collect(b, n, par):
        slot = lax.rem(b, 2)
        for r in range(0, STOK, 64):
            rows = slice(r, r + 64)
            acc_s = jnp.zeros((64, 128), jnp.float32) if n == 0 else acc_ref[0, rows, :]
            acc_t = jnp.zeros((64, 128), jnp.float32) if n == 0 else acc_ref[1, rows, :]
            for q in range(COL // 128):
                zq = z_refs[par][rows, q * 128:(q + 1) * 128]
                tq = tea_buf[slot, rows, n * COL + q * 128:n * COL + (q + 1) * 128].astype(jnp.float32)
                acc_s += jnp.exp2(jnp.tanh(zq * INV_CAP) * EXP_SCALE)
                acc_t += jnp.exp2(jnp.tanh(tq * INV_CAP) * EXP_SCALE)
            acc_ref[0, rows, :] = acc_s
            acc_ref[1, rows, :] = acc_t

    @pl.when(blocks > 0)
    def _():
        gather(0)
        logits(0, 0, 0)

    def block(b, _):
        @pl.when(b + 1 < blocks)
        def _():
            tea_start(b + 1)

        tea_wait(b)
        gather(b + 1)
        for n in range(count):
            if n + 1 < count:
                logits(b, n + 1, (n + 1) % 2)
            else:
                logits(b + 1, 0, 0)
            collect(b, n, n % 2)
        for k in range(per):
            dst = pl.ds(pl.multiple_of(order[b * per + k] * RUN, RUN), RUN)
            for s in range(2):
                sum_ref[s, dst, :] = acc_ref[s, k * RUN:(k + 1) * RUN, :]
        return 0

    lax.fori_loop(0, blocks, block, 0)

    def lines(i, _):
        for s in range(2):
            for b in range(8):
                rows = pl.ds(pl.multiple_of((i * 8 + b) * 128, 128), 128)
                out_ref[s * (tokens // 128) + i * 8 + b, :] = jnp.sum(sum_ref[s, rows, :].T, axis=0)
        return 0

    lax.fori_loop(0, tokens // 1024, lines, 0)
    x_out.wait()
    xt_out.wait()


def stats_call(mask_lines, gain_row, hid_t, tab_t, tea_rows):
    dim, tokens = hid_t.shape
    cols = tab_t.shape[1]
    assert (cols // COL) % 2 == 0
    hbm = pl.BlockSpec(memory_space=pl.ANY)
    vmem = pl.BlockSpec(memory_space=pltpu.VMEM)
    per = STOK // RUN
    return pl.pallas_call(
        stats_kernel,
        in_specs=[vmem, vmem, hbm, hbm, hbm],
        out_specs=[hbm, hbm, vmem],
        out_shape=[
            jax.ShapeDtypeStruct((tokens, dim), jnp.bfloat16),
            jax.ShapeDtypeStruct((dim, tokens), jnp.bfloat16),
            jax.ShapeDtypeStruct((tokens // 64, 128), jnp.float32),
        ],
        scratch_shapes=[
            pltpu.VMEM((dim, tokens), jnp.bfloat16),
            pltpu.VMEM((tokens, dim), jnp.bfloat16),
            pltpu.VMEM((dim, tokens), jnp.bfloat16),
            pltpu.VMEM((dim, cols), jnp.bfloat16),
            pltpu.VMEM((2, STOK, cols), jnp.bfloat16),
            pltpu.VMEM((2, STOK, dim), jnp.bfloat16),
            pltpu.VMEM((STOK, COL), jnp.float32),
            pltpu.VMEM((STOK, COL), jnp.float32),
            pltpu.VMEM((2, STOK, 128), jnp.float32),
            pltpu.VMEM((2, tokens, 128), jnp.float32),
            pltpu.VMEM((dim, 128), jnp.float32),
            pltpu.VMEM((tokens // 128, 128), jnp.int32),
            pltpu.SMEM((tokens // 128, 128), jnp.int32),
            pltpu.SMEM((tokens // RUN + 2 * per,), jnp.int32),
            pltpu.SemaphoreType.DMA((tokens // TOK,)),
            pltpu.SemaphoreType.DMA,
            pltpu.SemaphoreType.DMA((2,)),
            pltpu.SemaphoreType.DMA,
            pltpu.SemaphoreType.DMA((2,)),
        ],
        compiler_params=pltpu.CompilerParams(vmem_limit_bytes=VMEM_LIMIT),
        cost_estimate=pl.CostEstimate(flops=2 * tokens * cols * dim, bytes_accessed=2 * tokens * cols, transcendentals=0),
        name="stats",
    )(mask_lines, gain_row, hid_t, tab_t, tea_rows)


def first_kernel(tp, stats_ref, mask_ref, x_hbm, xt_hbm, tab_hbm, tea_hbm, ab_ref, log_ref, table_ref, g_ref, kl_ref,
                 slots, mask_slot, x_buf, xt_buf, tab_buf, tea_buf, z0_ref, z1_ref, stu_ref, tea_ref, gap_ref, coef0_ref, coef1_ref,
                 send_sem, recv_sem, msend_sem, mrecv_sem, x_sem, xt_sem, tab_sem, tea_sem):
    dp_me = lax.axis_index("dp")
    me = lax.axis_index("tp")
    tokens, width = g_ref.shape
    blocks = tokens // TOK

    def x_copy(m):
        rows = pl.ds(m * TOK, TOK)
        return pltpu.make_async_copy(x_hbm.at[rows, :], x_buf.at[rows, :], x_sem.at[m])

    tab_copy = pltpu.make_async_copy(tab_hbm.at[:, pl.ds(0, width)], tab_buf, tab_sem)
    tea_copy = pltpu.make_async_copy(tea_hbm.at[:, pl.ds(0, width)], tea_buf, tea_sem)
    xt_copy = pltpu.make_async_copy(xt_hbm, xt_buf, xt_sem)
    tab_copy.start()
    x_copy(0).start()
    tea_copy.start()
    for m in range(1, blocks):
        x_copy(m).start()
    xt_copy.start()

    barrier = pltpu.get_barrier_semaphore()
    for d in range(1, tp):
        pl.semaphore_signal(barrier, inc=1, device_id=(dp_me, lax.rem(me + d, tp)), device_id_type=MESH)
    pl.semaphore_signal(barrier, inc=1, device_id=(1 - dp_me, me), device_id_type=MESH)
    pl.semaphore_wait(barrier, tp)
    copies = []
    for d in range(1, tp):
        copies.append(pltpu.make_async_remote_copy(
            src_ref=stats_ref, dst_ref=slots.at[me], send_sem=send_sem.at[d], recv_sem=recv_sem.at[d],
            device_id=(dp_me, lax.rem(me + d, tp)), device_id_type=MESH))
    copies.append(pltpu.make_async_remote_copy(
        src_ref=mask_ref, dst_ref=mask_slot, send_sem=msend_sem, recv_sem=mrecv_sem,
        device_id=(1 - dp_me, me), device_id_type=MESH))
    for copy in copies:
        copy.start()
    slots[me] = stats_ref[...]

    z_refs = (z0_ref, z1_ref)

    def logits(m, par):
        rows = pl.ds(pl.multiple_of(m * TOK, TOK), TOK)
        z_refs[par][...] = lax.dot_general(x_buf[rows, :], tab_buf[...], NN, preferred_element_type=jnp.float32)

    def terms(m, par):
        for r in range(0, TOK, 64):
            rows = pl.ds(pl.multiple_of(m * TOK + r, 64), 64)
            gap = jnp.zeros((64, 128), jnp.float32)
            for q in range(width // 128):
                lanes = slice(q * 128, (q + 1) * 128)
                ts = jnp.tanh(z_refs[par][r:r + 64, lanes] * INV_CAP)
                tt = jnp.tanh(tea_buf[rows, lanes].astype(jnp.float32) * INV_CAP)
                slope = 1.0 - ts * ts
                eb = jnp.exp2(tt * EXP_SCALE)
                stu_ref[rows, lanes] = jnp.exp2(ts * EXP_SCALE) * slope
                tea_ref[rows, lanes] = eb * slope
                gap += eb * (tt - ts)
            gap_ref[rows, :] = gap

    tab_copy.wait()
    x_copy(0).wait()
    tea_copy.wait()
    logits(0, 0)

    def ahead(p, _):
        for par in range(2):
            m = 2 * p + par
            pltpu.make_async_copy(x_hbm.at[pl.ds(0, TOK), :], x_buf.at[pl.ds(0, TOK), :], x_sem.at[m + 1]).wait()
            logits(m + 1, 1 - par)
            terms(m, par)
        return 0

    if blocks > 2:
        lax.fori_loop(0, blocks // 2 - 1, ahead, 0)
    x_copy(blocks - 1).wait()
    logits(blocks - 1, 1)
    terms(blocks - 2, 0)
    terms(blocks - 1, 1)

    xt_copy.wait()
    for copy in copies:
        copy.wait()
    total = slots[0]
    for k in range(1, tp):
        total += slots[k]
    mask = mask_ref[...]
    weight = mask / (jnp.sum(mask, keepdims=True) + jnp.sum(mask_slot[...], keepdims=True))
    half = mask.shape[0]
    ab_ref[:half, :] = weight / total[:half]
    ab_ref[half:, :] = weight / total[half:]
    logs = weight * (jnp.log(total[:half]) - jnp.log(total[half:]))
    log_ref[...] = jnp.sum(logs.reshape(-1, 8, 128), axis=0)

    kl_ref[...] = jnp.zeros_like(kl_ref)
    table_ref[...] = jnp.zeros_like(table_ref)
    coef_refs = (coef0_ref, coef1_ref)

    def spread(m, par):
        for k in range(2):
            for b in range(LINES):
                line = ab_ref[pl.ds(k * half + m * LINES + b, 1), :]
                coef_refs[par][k, b * 128:(b + 1) * 128, :] = jnp.broadcast_to(line, (128, 128)).T

    def weigh(m, par):
        kl_acc = kl_ref[...]
        for r in range(0, TOK, 64):
            rows = pl.ds(pl.multiple_of(m * TOK + r, 64), 64)
            a = coef_refs[par][0, r:r + 64, :]
            b = coef_refs[par][1, r:r + 64, :]
            gap = gap_ref[rows, :] * b
            for w in range(0, 64, 8):
                kl_acc += gap[w:w + 8]
            for q in range(width // 128):
                lanes = slice(q * 128, (q + 1) * 128)
                g_ref[rows, lanes] = (stu_ref[rows, lanes] * a - tea_ref[rows, lanes] * b).astype(jnp.bfloat16)
        kl_ref[...] = kl_acc

    def product(m):
        rows = pl.ds(pl.multiple_of(m * TOK, TOK), TOK)
        table_ref[...] += lax.dot_general(xt_buf[:, rows], g_ref[rows, :], NN, preferred_element_type=jnp.float32)

    spread(0, 0)
    spread(1, 1)
    weigh(0, 0)

    def behind(p, _):
        for par in range(2):
            m = 2 * p + par
            spread(m, par)
            weigh(m - 1, 1 - par)
            product(m - 2)
        return 0

    lax.fori_loop(1, blocks // 2, behind, 0)
    weigh(blocks - 1, 1)
    product(blocks - 2)
    product(blocks - 1)


def first_call(stats, mask_lines, x_rows, x_t, tab_t, tea_rows, width, tp):
    tokens, dim = x_rows.shape
    whole = pl.BlockSpec(memory_space=pltpu.VMEM)
    hbm = pl.BlockSpec(memory_space=pl.ANY)
    blocks = tokens // TOK
    return pl.pallas_call(
        functools.partial(first_kernel, tp),
        in_specs=[whole, whole, hbm, hbm, hbm, hbm],
        out_specs=[whole] * 5,
        out_shape=[
            jax.ShapeDtypeStruct(stats.shape, jnp.float32),
            jax.ShapeDtypeStruct((8, 128), jnp.float32),
            jax.ShapeDtypeStruct((dim, width), jnp.float32),
            jax.ShapeDtypeStruct((tokens, width), jnp.bfloat16),
            jax.ShapeDtypeStruct((8, 128), jnp.float32),
        ],
        scratch_shapes=[
            pltpu.VMEM((tp,) + stats.shape, jnp.float32),
            pltpu.VMEM(mask_lines.shape, jnp.float32),
            pltpu.VMEM((tokens, dim), jnp.bfloat16),
            pltpu.VMEM((dim, tokens), jnp.bfloat16),
            pltpu.VMEM((dim, width), jnp.bfloat16),
            pltpu.VMEM((tokens, width), jnp.bfloat16),
            pltpu.VMEM((TOK, width), jnp.float32),
            pltpu.VMEM((TOK, width), jnp.float32),
            pltpu.VMEM((tokens, width), jnp.float32),
            pltpu.VMEM((tokens, width), jnp.float32),
            pltpu.VMEM((tokens, 128), jnp.float32),
            pltpu.VMEM((2, TOK, 128), jnp.float32),
            pltpu.VMEM((2, TOK, 128), jnp.float32),
            pltpu.SemaphoreType.DMA((tp,)),
            pltpu.SemaphoreType.DMA((tp,)),
            pltpu.SemaphoreType.DMA,
            pltpu.SemaphoreType.DMA,
            pltpu.SemaphoreType.DMA((blocks,)),
            pltpu.SemaphoreType.DMA,
            pltpu.SemaphoreType.DMA,
            pltpu.SemaphoreType.DMA,
        ],
        compiler_params=pltpu.CompilerParams(collective_id=0, has_side_effects=True, vmem_limit_bytes=VMEM_LIMIT),
        cost_estimate=pl.CostEstimate(flops=4 * tokens * width * dim, bytes_accessed=4 * tokens * dim, transcendentals=0),
        name="first",
    )(stats, mask_lines, x_rows, x_t, tab_t, tea_rows)


def grad_kernel(first, ab_ref, x_ref, xt_ref, tab_ref, tea_ref, *refs):
    if first:
        table_ref, g_ref, kl_ref, z0_ref, z1_ref, coef_ref = refs
    else:
        kl_in_ref, table_ref, g_ref, kl_ref, z0_ref, z1_ref, coef_ref = refs
    z_refs = (z0_ref, z1_ref)
    col = z0_ref.shape[1]
    count = tab_ref.shape[1] // col
    block = pl.program_id(0)

    @pl.when(block == 0)
    def _():
        table_ref[...] = jnp.zeros_like(table_ref)
        kl_ref[...] = jnp.zeros_like(kl_ref) if first else kl_in_ref[...]

    for k in range(2):
        for b in range(LINES):
            line = ab_ref[pl.ds(k * (ab_ref.shape[0] // 2) + block * LINES + b, 1), :]
            coef_ref[k, b * 128:(b + 1) * 128, :] = jnp.broadcast_to(line, (128, 128)).T

    def columns(n):
        return pl.ds(pl.multiple_of(n * col, col), col)

    def logits(n, par):
        z_refs[par][...] = lax.dot_general(x_ref[...], tab_ref[:, columns(n)], NN, preferred_element_type=jnp.float32)

    def weigh(n, par):
        kl_acc = kl_ref[...]
        for r in range(0, TOK, 64):
            rows = slice(r, r + 64)
            a = coef_ref[0, rows, :]
            b = coef_ref[1, rows, :]
            for q in range(col // 128):
                lanes = pl.ds(pl.multiple_of(n * col + q * 128, 128), 128)
                zq = z_refs[par][rows, q * 128:(q + 1) * 128]
                tq = tea_ref[rows, lanes].astype(jnp.float32)
                ts = jnp.tanh(zq * INV_CAP)
                tt = jnp.tanh(tq * INV_CAP)
                pa = jnp.exp2(ts * EXP_SCALE) * a
                pb = jnp.exp2(tt * EXP_SCALE) * b
                kl = pb * (tt - ts)
                for w in range(0, 64, 8):
                    kl_acc += kl[w:w + 8]
                g_ref[rows, lanes] = ((pa - pb) * (1.0 - ts * ts)).astype(jnp.bfloat16)
        kl_ref[...] = kl_acc

    def product(n):
        table_ref[:, columns(n)] += lax.dot_general(xt_ref[...], g_ref[:, columns(n)], NN, preferred_element_type=jnp.float32)

    logits(0, 0)
    if count == 1:
        weigh(0, 0)
        product(0)
        return
    logits(1, 1)
    weigh(0, 0)

    def pair(p, _):
        for par in range(2):
            n = 2 * p + par
            logits(n, par)
            weigh(n - 1, 1 - par)
            product(n - 2)
        return 0

    if count == 4:
        pair(1, 0)
    elif count > 4:
        lax.fori_loop(1, count // 2, pair, 0)
    product(count - 2)
    weigh(count - 1, 1)
    product(count - 1)


def grad_call(ab, x_rows, x_t, tab_t, tea_rows, start, size, kl):
    tokens, dim = x_rows.shape
    first = kl is None
    col = min(GCOL, size)
    assert size == col or size % (2 * col) == 0
    in_specs = [
        pl.BlockSpec(ab.shape, lambda i: (0, 0)),
        pl.BlockSpec((TOK, dim), lambda i: (i, 0)),
        pl.BlockSpec((dim, TOK), lambda i: (0, i)),
        pl.BlockSpec((pl.Element(dim), pl.Element(size)), lambda i: (0, start), pipeline_mode=pl.Buffered(1)),
        pl.BlockSpec((pl.Element(TOK), pl.Element(size)), lambda i: (i * TOK, start)),
    ]
    operands = [ab, x_rows, x_t, tab_t, tea_rows]
    if not first:
        in_specs.append(pl.BlockSpec((8, 128), lambda i: (0, 0)))
        operands.append(kl)
    return pl.pallas_call(
        functools.partial(grad_kernel, first),
        grid=(tokens // TOK,),
        in_specs=in_specs,
        out_specs=[
            pl.BlockSpec((dim, size), lambda i: (0, 0)),
            pl.BlockSpec((TOK, size), lambda i: (i, 0)),
            pl.BlockSpec((8, 128), lambda i: (0, 0)),
        ],
        out_shape=[
            jax.ShapeDtypeStruct((dim, size), jnp.float32),
            jax.ShapeDtypeStruct((tokens, size), jnp.bfloat16),
            jax.ShapeDtypeStruct((8, 128), jnp.float32),
        ],
        scratch_shapes=[
            pltpu.VMEM((TOK, col), jnp.float32),
            pltpu.VMEM((TOK, col), jnp.float32),
            pltpu.VMEM((2, TOK, 128), jnp.float32),
        ],
        compiler_params=pltpu.CompilerParams(vmem_limit_bytes=VMEM_LIMIT),
        cost_estimate=pl.CostEstimate(flops=4 * tokens * size * dim, bytes_accessed=4 * tokens * size, transcendentals=0),
    )(*operands)


def back_kernel(half_ref, tab_ref, *refs):
    g_refs, dx_ref = refs[:-1], refs[-1]
    start = 0
    for g_ref in g_refs:
        size = g_ref.shape[1]
        step = min(BACK, size)
        for n in range(size // step):
            cols = slice(start + n * step, start + (n + 1) * step)
            dx = lax.dot_general(tab_ref[:, cols], g_ref[:, n * step:(n + 1) * step], NT, preferred_element_type=jnp.float32)
            if start + n == 0:
                dx_ref[...] = dx
            else:
                dx_ref[...] += dx
        start += size


def back_call(tab_t, grads, half):
    dim, cols = tab_t.shape
    tokens = grads[0].shape[0]
    rows = dim // 2
    return pl.pallas_call(
        back_kernel,
        grid_spec=pltpu.PrefetchScalarGridSpec(
            num_scalar_prefetch=1,
            grid=(tokens // TOK,),
            in_specs=[pl.BlockSpec((rows, cols), lambda i, h: (h[0], 0), pipeline_mode=pl.Buffered(1))]
            + [pl.BlockSpec((TOK, g.shape[1]), lambda i, h: (i, 0)) for g in grads],
            out_specs=pl.BlockSpec((rows, TOK), lambda i, h: (0, i)),
        ),
        out_shape=jax.ShapeDtypeStruct((rows, tokens), jnp.float32),
        compiler_params=pltpu.CompilerParams(vmem_limit_bytes=VMEM_LIMIT),
        cost_estimate=pl.CostEstimate(flops=tokens * cols * dim, bytes_accessed=2 * tokens * cols, transcendentals=0),
        name="back",
    )(half[None], tab_t, *grads)


def finish_kernel(off_ref, hid_ref, gain_ref, *refs):
    piece_refs, (out_ref, sum_ref, norm_ref, a_ref, gain_buf) = refs[:-5], refs[-5:]
    dim, toks = hid_ref.shape

    @pl.when(pl.program_id(0) == 0)
    def _():
        gain_buf[...] = jnp.broadcast_to(1.0 + gain_ref[...], (128, dim)).T
        sum_ref[...] = jnp.zeros_like(sum_ref)

    hid = hid_ref[...].astype(jnp.float32)
    inv_rms = lax.rsqrt(jnp.mean(hid * hid, axis=0, keepdims=True) + NORM_EPS)
    norm_ref[...] = hid * inv_rms
    dot = jnp.zeros((1, toks), jnp.float32)
    for k, piece_ref in enumerate(piece_refs):
        rows = pl.ds(pl.multiple_of(off_ref[k], 8), piece_ref.shape[0])
        gain = gain_buf[rows, :]
        acc = sum_ref[rows, :]
        for b in range(toks // 128):
            lanes = slice(b * 128, (b + 1) * 128)
            a_ref[rows, lanes] = piece_ref[:, lanes] * gain
            acc += piece_ref[:, lanes] * norm_ref[rows, lanes]
        sum_ref[rows, :] = acc
        dot += jnp.sum(a_ref[rows, :] * norm_ref[rows, :], axis=0, keepdims=True)
    out_ref[...] = (inv_rms * (a_ref[...] - norm_ref[...] * (dot / dim))).astype(jnp.bfloat16)


def finish_call(offsets, hid_t, gain_row, pieces):
    dim, tokens = hid_t.shape
    rows = pieces[0].shape[0]
    return pl.pallas_call(
        finish_kernel,
        grid_spec=pltpu.PrefetchScalarGridSpec(
            num_scalar_prefetch=1,
            grid=(tokens // TOK,),
            in_specs=[pl.BlockSpec((dim, TOK), lambda i, o: (0, i)), pl.BlockSpec((1, dim), lambda i, o: (0, 0))]
            + [pl.BlockSpec((rows, TOK), lambda i, o: (0, i))] * len(pieces),
            out_specs=[pl.BlockSpec((dim, TOK), lambda i, o: (0, i)), pl.BlockSpec((dim, 128), lambda i, o: (0, 0))],
            scratch_shapes=[pltpu.VMEM((dim, TOK), jnp.float32), pltpu.VMEM((dim, TOK), jnp.float32), pltpu.VMEM((dim, 128), jnp.float32)],
        ),
        out_shape=[jax.ShapeDtypeStruct((dim, tokens), jnp.bfloat16), jax.ShapeDtypeStruct((dim, 128), jnp.float32)],
        compiler_params=pltpu.CompilerParams(vmem_limit_bytes=VMEM_LIMIT),
        cost_estimate=pl.CostEstimate(flops=10 * tokens * dim, bytes_accessed=8 * tokens * dim, transcendentals=0),
        name="finish",
    )(offsets, hid_t, gain_row, *pieces)


def add_kernel(own_ref, recv_ref, *refs):
    refs[-1][...] = own_ref[...] + recv_ref[...]


def add_call(own, recv, start, cols, out, after):
    dim, size = own.shape
    step = 128
    spec = pl.BlockSpec((dim, step), lambda i: (0, i))
    hold = pl.BlockSpec(memory_space=pl.ANY)
    in_specs = [spec, spec]
    operands = [own, recv]
    aliases = {}
    if out is not None:
        operands.append(out)
        aliases = {2: 0}
    operands += after
    in_specs += [hold] * (len(operands) - 2)
    return pl.pallas_call(
        add_kernel,
        grid=(size // step,),
        in_specs=in_specs,
        out_specs=pl.BlockSpec((dim, step), lambda i: (0, start // step + i)),
        out_shape=jax.ShapeDtypeStruct((dim, cols), jnp.float32),
        input_output_aliases=aliases,
        cost_estimate=pl.CostEstimate(flops=size * dim, bytes_accessed=12 * size * dim, transcendentals=0),
    )(*operands)


def exchange_partner(i, step):
    if step == 0:
        return i ^ 1
    return i ^ (2 if (i & 1) == (step - 1) else 4)


def place(bits, rows):
    return (bits[0] * (rows // 2) + bits[1] * (rows // 4) + bits[2] * (rows // 8)).astype(jnp.int32)


def solution(mesh):
    tp = mesh.shape["tp"]

    def local_step(hid_rows, w_final, tab_rows, tea_rows, mask_rows):
        tokens, dim = hid_rows.shape
        hid_t, tab_t = hid_rows.T, tab_rows.T
        mask_lines = mask_rows.reshape(tokens // 128, 128)
        x_rows, x_t, stats = stats_call(mask_lines, w_final.reshape(1, dim), hid_t, tab_t, tea_rows)

        swap = [(0, 1), (1, 0)]
        start = 0
        parts, grads = [], []
        for c, size in enumerate(CHUNKS):
            if c == 0:
                ab, log_part, table_c, g, kl = first_call(stats, mask_lines, x_rows, x_t, tab_t, tea_rows, size, tp)
            else:
                table_c, g, kl = grad_call(ab, x_rows, x_t, tab_t, tea_rows, start, size, kl)
            grads.append(g)
            recv = lax.ppermute(table_c, "dp", swap)
            parts.append((start, table_c, recv))
            start += size

        me = lax.axis_index("tp")
        core, xb, yb = me & 1, (me >> 1) & 1, (me >> 2) & 1
        bits = (core, jnp.where(core == 0, xb, yb), jnp.where(core == 0, yb, xb))
        perms = [[(i, exchange_partner(i, s)) for i in range(tp)] for s in range(3)]
        away = back_call(tab_t, grads, 1 - core)
        recv = lax.ppermute(away, "tp", perms[0])
        keep = back_call(tab_t, grads, core)
        for s in (1, 2):
            half = keep.shape[0] // 2
            gone = (1 - bits[s]) * half
            away = lax.dynamic_slice_in_dim(keep, gone, half, 0) + lax.dynamic_slice_in_dim(recv, gone, half, 0)
            away = lax.ppermute(away, "tp", perms[s])
            kept = bits[s] * half
            keep = lax.dynamic_slice_in_dim(keep, kept, half, 0) + lax.dynamic_slice_in_dim(recv, kept, half, 0)
            recv = away
        own = keep + recv
        pieces = [own]
        for s in (2, 1, 0):
            pieces += [lax.ppermute(piece, "tp", perms[s]) for piece in pieces]
        c, u, v = bits
        spots = [(c, u, v), (c, u, 1 - v), (c, 1 - u, v), (c, 1 - u, 1 - v)]
        spots += [(1 - c, v, u), (1 - c, v, 1 - u), (1 - c, 1 - v, u), (1 - c, 1 - v, 1 - u)]
        offsets = jnp.stack([place(spot, dim) for spot in spots])

        loss_part = lax.psum(SOFT_CAP * jnp.sum(kl), "tp") + jnp.sum(log_part)
        grad_h, gain_part = finish_call(offsets, hid_t, w_final.reshape(1, dim), pieces)
        small = jnp.concatenate([jnp.sum(gain_part, axis=1), jnp.full((1024 - dim,), loss_part)])
        other = lax.ppermute(small, "dp", swap)
        small = small + other

        out = None
        for n, (begin, own, recv) in enumerate(parts):
            last = n == len(parts) - 1
            out = add_call(own, recv, begin, tab_t.shape[1], out, [grad_h, small] if last else [])
        return small[dim], grad_h.T, small[:dim], out.T

    return jax.shard_map(local_step, mesh=mesh, in_specs=(P('dp', None), P(None), P('tp', None), P('dp', 'tp'), P('dp')), out_specs=(P(), P('dp', None), P(None), P('tp', None)), check_vma=False)
```

```python
import functools

import jax
import jax.numpy as jnp
from jax import lax
from jax.experimental import pallas as pl
from jax.experimental.pallas import tpu as pltpu
from jax.sharding import PartitionSpec as P


SOFT_CAP = 30.0
NORM_EPS = 1e-6
INV_CAP = 1.0 / SOFT_CAP
EXP_SCALE = SOFT_CAP * 1.4426950408889634
TOK = 512
LINES = TOK // 128
RUN = 16
STOK = 256
COL = 512
GCOL = 256
CHUNKS = (256, 256, 512, 1024, 2048, 1536, 384, 128)
VMEM_LIMIT = 62 * 1024 * 1024
MESH = pl.DeviceIdType.MESH
NT = (((1,), (1,)), ((), ()))
NN = (((1,), (0,)), ((), ()))


def stats_kernel(mask_hbm, gain_hbm, hid_hbm, tab_hbm, tea_hbm, x_hbm, xt_hbm, out_ref,
                 mask_buf, row_buf, hid_buf, x_buf, xt_buf, tab_buf, tea_buf, rows_ref, z0_ref, z1_ref, acc_ref, sum_ref, gain_buf, flag_buf,
                 flags, order, hid_sem, tab_sem, tea_sem, flag_sem, row_sem, out_sem):
    z_refs = (z0_ref, z1_ref)
    dim, tokens = hid_hbm.shape
    count = tab_hbm.shape[1] // COL
    slabs = tokens // TOK
    runs = tokens // RUN
    per = STOK // RUN

    def hid_copy(i):
        cols = pl.ds(i * TOK, TOK)
        return pltpu.make_async_copy(hid_hbm.at[:, cols], hid_buf.at[:, cols], hid_sem.at[i])

    def tab_copy(i):
        cols = pl.ds(i * COL, COL)
        return pltpu.make_async_copy(tab_hbm.at[:, cols], tab_buf.at[:, cols], tab_sem)

    mask_copy = pltpu.make_async_copy(mask_hbm, mask_buf, flag_sem)
    row_copy = pltpu.make_async_copy(gain_hbm, row_buf, row_sem)
    mask_copy.start()
    row_copy.start()
    for i in range(slabs):
        hid_copy(i).start()
    for i in range(count):
        tab_copy(i).start()

    mask_copy.wait()
    flag = mask_buf[...]
    for shift in (1, 2, 4, 8):
        flag = jnp.maximum(flag, pltpu.roll(flag, 128 - shift, 1))
    flag_buf[...] = (flag > 0).astype(jnp.int32)
    flag_copy = pltpu.make_async_copy(flag_buf, flags, flag_sem)
    flag_copy.start()
    row_copy.wait()
    gain_buf[...] = jnp.broadcast_to(1.0 + row_buf[...], (128, dim)).T
    sum_ref[...] = jnp.ones_like(sum_ref)
    flag_copy.wait()

    def tea_start(b):
        slot = lax.rem(b, 2)

        def one(k, _):
            src = pl.ds(pl.multiple_of(order[b * per + k] * RUN, RUN), RUN)
            dst = pl.ds(pl.multiple_of(k * RUN, RUN), RUN)
            pltpu.make_async_copy(tea_hbm.at[src, :], tea_buf.at[slot, dst, :], tea_sem.at[slot]).start()
            return 0

        lax.fori_loop(0, per, one, 0)

    def tea_wait(b):
        slot = lax.rem(b, 2)
        pltpu.make_async_copy(tea_hbm.at[pl.ds(0, STOK), :], tea_buf.at[slot], tea_sem.at[slot]).wait()

    def slab(i, found, marks):
        pltpu.make_async_copy(hid_hbm.at[:, pl.ds(0, TOK)], hid_buf.at[:, pl.ds(0, TOK)], hid_sem.at[i]).wait()
        for r in range(marks):
            run = i * marks + r
            order[found] = run
            found = found + flags[lax.div(i * marks, 128 // RUN) + r // (128 // RUN), r % (128 // RUN) * RUN]
        for b in range(LINES):
            lanes = pl.ds(pl.multiple_of(i * TOK + b * 128, 128), 128)
            hid = hid_buf[:, lanes].astype(jnp.float32)
            inv_rms = lax.rsqrt(jnp.mean(hid * hid, axis=0, keepdims=True) + NORM_EPS)
            xb = (hid * inv_rms * gain_buf[...]).astype(jnp.bfloat16)
            xt_buf[:, lanes] = xb
            x_buf[lanes, :] = xb.T
        return found

    early = slabs // 2
    found = lax.fori_loop(0, early, lambda i, found: slab(i, found, runs // early), 0)
    last = order[jnp.maximum(found - 1, 0)]
    last = jnp.where(found > 0, last, 0)
    for k in range(2 * per):
        order[found + k] = last
    blocks = lax.div(found + per - 1, per)

    @pl.when(blocks > 0)
    def _():
        tea_start(0)

    lax.fori_loop(early, slabs, lambda i, _: slab(i, 0, 0), 0)
    x_out = pltpu.make_async_copy(x_buf, x_hbm, out_sem.at[0])
    xt_out = pltpu.make_async_copy(xt_buf, xt_hbm, out_sem.at[1])
    x_out.start()
    xt_out.start()
    pltpu.make_async_copy(tab_hbm, tab_buf, tab_sem).wait()

    def gather(b):
        slot = lax.rem(b, 2)
        for k in range(per):
            src = pl.ds(pl.multiple_of(order[b * per + k] * RUN, RUN), RUN)
            rows_ref[slot, k * RUN:(k + 1) * RUN, :] = x_buf[src, :]

    def logits(b, n, par):
        cols = slice(n * COL, (n + 1) * COL)
        z_refs[par][...] = lax.dot_general(rows_ref[lax.rem(b, 2)], tab_buf[:, cols], NN, preferred_element_type=jnp.float32)

    def collect(b, n, par):
        slot = lax.rem(b, 2)
        for r in range(0, STOK, 64):
            rows = slice(r, r + 64)
            acc_s = jnp.zeros((64, 128), jnp.float32) if n == 0 else acc_ref[0, rows, :]
            acc_t = jnp.zeros((64, 128), jnp.float32) if n == 0 else acc_ref[1, rows, :]
            for q in range(COL // 128):
                zq = z_refs[par][rows, q * 128:(q + 1) * 128]
                tq = tea_buf[slot, rows, n * COL + q * 128:n * COL + (q + 1) * 128].astype(jnp.float32)
                acc_s += jnp.exp2(jnp.tanh(zq * INV_CAP) * EXP_SCALE)
                acc_t += jnp.exp2(jnp.tanh(tq * INV_CAP) * EXP_SCALE)
            acc_ref[0, rows, :] = acc_s
            acc_ref[1, rows, :] = acc_t

    @pl.when(blocks > 0)
    def _():
        gather(0)
        logits(0, 0, 0)

    def block(b, _):
        @pl.when(b + 1 < blocks)
        def _():
            tea_start(b + 1)

        tea_wait(b)
        for n in range(count):
            if n + 1 < count:
                logits(b, n + 1, (n + 1) % 2)
            else:
                gather(b + 1)
                logits(b + 1, 0, 0)
            collect(b, n, n % 2)
        for k in range(per):
            dst = pl.ds(pl.multiple_of(order[b * per + k] * RUN, RUN), RUN)
            for s in range(2):
                sum_ref[s, dst, :] = acc_ref[s, k * RUN:(k + 1) * RUN, :]
        return 0

    lax.fori_loop(0, blocks, block, 0)

    def lines(i, _):
        for s in range(2):
            for b in range(8):
                rows = pl.ds(pl.multiple_of((i * 8 + b) * 128, 128), 128)
                out_ref[s * (tokens // 128) + i * 8 + b, :] = jnp.sum(sum_ref[s, rows, :].T, axis=0)
        return 0

    lax.fori_loop(0, tokens // 1024, lines, 0)
    x_out.wait()
    xt_out.wait()


def stats_call(mask_lines, gain_row, hid_t, tab_t, tea_rows):
    dim, tokens = hid_t.shape
    cols = tab_t.shape[1]
    assert (cols // COL) % 2 == 0
    hbm = pl.BlockSpec(memory_space=pl.ANY)
    vmem = pl.BlockSpec(memory_space=pltpu.VMEM)
    per = STOK // RUN
    return pl.pallas_call(
        stats_kernel,
        in_specs=[hbm] * 5,
        out_specs=[hbm, hbm, vmem],
        out_shape=[
            jax.ShapeDtypeStruct((tokens, dim), jnp.bfloat16),
            jax.ShapeDtypeStruct((dim, tokens), jnp.bfloat16),
            jax.ShapeDtypeStruct((tokens // 64, 128), jnp.float32),
        ],
        scratch_shapes=[
            pltpu.VMEM(mask_lines.shape, jnp.float32),
            pltpu.VMEM((1, dim), jnp.float32),
            pltpu.VMEM((dim, tokens), jnp.bfloat16),
            pltpu.VMEM((tokens, dim), jnp.bfloat16),
            pltpu.VMEM((dim, tokens), jnp.bfloat16),
            pltpu.VMEM((dim, cols), jnp.bfloat16),
            pltpu.VMEM((2, STOK, cols), jnp.bfloat16),
            pltpu.VMEM((2, STOK, dim), jnp.bfloat16),
            pltpu.VMEM((STOK, COL), jnp.float32),
            pltpu.VMEM((STOK, COL), jnp.float32),
            pltpu.VMEM((2, STOK, 128), jnp.float32),
            pltpu.VMEM((2, tokens, 128), jnp.float32),
            pltpu.VMEM((dim, 128), jnp.float32),
            pltpu.VMEM((tokens // 128, 128), jnp.int32),
            pltpu.SMEM((tokens // 128, 128), jnp.int32),
            pltpu.SMEM((tokens // RUN + 2 * per,), jnp.int32),
            pltpu.SemaphoreType.DMA((tokens // TOK,)),
            pltpu.SemaphoreType.DMA,
            pltpu.SemaphoreType.DMA((2,)),
            pltpu.SemaphoreType.DMA,
            pltpu.SemaphoreType.DMA,
            pltpu.SemaphoreType.DMA((2,)),
        ],
        compiler_params=pltpu.CompilerParams(vmem_limit_bytes=VMEM_LIMIT),
        cost_estimate=pl.CostEstimate(flops=2 * tokens * cols * dim, bytes_accessed=2 * tokens * cols, transcendentals=0),
        name="stats",
    )(mask_lines, gain_row, hid_t, tab_t, tea_rows)


def first_kernel(tp, stats_hbm, mask_hbm, x_hbm, xt_hbm, tab_hbm, tea_hbm, ab_ref, log_ref, table_ref, g_hbm, kl_ref,
                 stats_ref, mask_ref, g_ref, slots, mask_slot, x_buf, xt_buf, tab_buf, tea_buf, z0_ref, z1_ref, stu_ref, tea_ref, gap_ref, coef0_ref, coef1_ref,
                 send_sem, recv_sem, msend_sem, mrecv_sem, stats_sem, mask_sem, x_sem, xt_sem, tab_sem, tea_sem, g_sem):
    dp_me = lax.axis_index("dp")
    me = lax.axis_index("tp")
    tokens, width = g_ref.shape
    blocks = tokens // TOK

    def g_copy(m):
        rows = pl.ds(pl.multiple_of(m * TOK, TOK), TOK)
        return pltpu.make_async_copy(g_ref.at[rows, :], g_hbm.at[rows, :], g_sem)

    def x_copy(m):
        rows = pl.ds(m * TOK, TOK)
        return pltpu.make_async_copy(x_hbm.at[rows, :], x_buf.at[rows, :], x_sem.at[m])

    tab_copy = pltpu.make_async_copy(tab_hbm.at[:, pl.ds(0, width)], tab_buf, tab_sem)
    tea_copy = pltpu.make_async_copy(tea_hbm.at[:, pl.ds(0, width)], tea_buf, tea_sem)
    xt_copy = pltpu.make_async_copy(xt_hbm, xt_buf, xt_sem)
    stats_copy = pltpu.make_async_copy(stats_hbm, stats_ref, stats_sem)
    mask_copy = pltpu.make_async_copy(mask_hbm, mask_ref, mask_sem)
    barrier = pltpu.get_barrier_semaphore()
    for d in range(1, tp):
        pl.semaphore_signal(barrier, inc=1, device_id=(dp_me, lax.rem(me + d, tp)), device_id_type=MESH)
    pl.semaphore_signal(barrier, inc=1, device_id=(1 - dp_me, me), device_id_type=MESH)
    stats_copy.start()
    mask_copy.start()
    tab_copy.start()
    x_copy(0).start()
    tea_copy.start()
    for m in range(1, blocks):
        x_copy(m).start()
    xt_copy.start()

    z_refs = (z0_ref, z1_ref)

    def logits(m, par):
        rows = pl.ds(pl.multiple_of(m * TOK, TOK), TOK)
        z_refs[par][...] = lax.dot_general(x_buf[rows, :], tab_buf[...], NN, preferred_element_type=jnp.float32)

    def terms(m, par):
        for r in range(0, TOK, 64):
            rows = pl.ds(pl.multiple_of(m * TOK + r, 64), 64)
            gap = jnp.zeros((64, 128), jnp.float32)
            for q in range(width // 128):
                lanes = slice(q * 128, (q + 1) * 128)
                ts = jnp.tanh(z_refs[par][r:r + 64, lanes] * INV_CAP)
                tt = jnp.tanh(tea_buf[rows, lanes].astype(jnp.float32) * INV_CAP)
                slope = 1.0 - ts * ts
                eb = jnp.exp2(tt * EXP_SCALE)
                stu_ref[rows, lanes] = jnp.exp2(ts * EXP_SCALE) * slope
                tea_ref[rows, lanes] = eb * slope
                gap += eb * (tt - ts)
            gap_ref[rows, :] = gap

    stats_copy.wait()
    mask_copy.wait()
    pl.semaphore_wait(barrier, tp)
    copies = []
    for d in range(1, tp):
        copies.append(pltpu.make_async_remote_copy(
            src_ref=stats_ref, dst_ref=slots.at[me], send_sem=send_sem.at[d], recv_sem=recv_sem.at[d],
            device_id=(dp_me, lax.rem(me + d, tp)), device_id_type=MESH))
    copies.append(pltpu.make_async_remote_copy(
        src_ref=mask_ref, dst_ref=mask_slot, send_sem=msend_sem, recv_sem=mrecv_sem,
        device_id=(1 - dp_me, me), device_id_type=MESH))
    for copy in copies:
        copy.start()
    slots[me] = stats_ref[...]
    tab_copy.wait()
    x_copy(0).wait()
    tea_copy.wait()
    logits(0, 0)

    def ahead(p, _):
        for par in range(2):
            m = 2 * p + par
            pltpu.make_async_copy(x_hbm.at[pl.ds(0, TOK), :], x_buf.at[pl.ds(0, TOK), :], x_sem.at[m + 1]).wait()
            logits(m + 1, 1 - par)
            terms(m, par)
        return 0

    if blocks > 2:
        lax.fori_loop(0, blocks // 2 - 1, ahead, 0)
    x_copy(blocks - 1).wait()
    logits(blocks - 1, 1)
    terms(blocks - 2, 0)
    terms(blocks - 1, 1)

    xt_copy.wait()
    for copy in copies:
        copy.wait()
    total = slots[0]
    for k in range(1, tp):
        total += slots[k]
    mask = mask_ref[...]
    weight = mask / (jnp.sum(mask, keepdims=True) + jnp.sum(mask_slot[...], keepdims=True))
    half = mask.shape[0]
    ab_ref[:half, :] = weight / total[:half]
    ab_ref[half:, :] = weight / total[half:]
    logs = weight * (jnp.log(total[:half]) - jnp.log(total[half:]))
    log_ref[...] = jnp.sum(logs.reshape(-1, 8, 128), axis=0)

    kl_ref[...] = jnp.zeros_like(kl_ref)
    table_ref[...] = jnp.zeros_like(table_ref)
    coef_refs = (coef0_ref, coef1_ref)

    def spread(m, par):
        for k in range(2):
            for b in range(LINES):
                line = ab_ref[pl.ds(k * half + m * LINES + b, 1), :]
                coef_refs[par][k, b * 128:(b + 1) * 128, :] = jnp.broadcast_to(line, (128, 128)).T

    def weigh(m, par):
        kl_acc = kl_ref[...]
        for r in range(0, TOK, 64):
            rows = pl.ds(pl.multiple_of(m * TOK + r, 64), 64)
            a = coef_refs[par][0, r:r + 64, :]
            b = coef_refs[par][1, r:r + 64, :]
            gap = gap_ref[rows, :] * b
            for w in range(0, 64, 8):
                kl_acc += gap[w:w + 8]
            for q in range(width // 128):
                lanes = slice(q * 128, (q + 1) * 128)
                g_ref[rows, lanes] = (stu_ref[rows, lanes] * a - tea_ref[rows, lanes] * b).astype(jnp.bfloat16)
        kl_ref[...] = kl_acc

    def product(m):
        rows = pl.ds(pl.multiple_of(m * TOK, TOK), TOK)
        table_ref[...] += lax.dot_general(xt_buf[:, rows], g_ref[rows, :], NN, preferred_element_type=jnp.float32)

    spread(0, 0)
    spread(1, 1)
    weigh(0, 0)

    def behind(p, _):
        for par in range(2):
            m = 2 * p + par
            spread(m, par)
            weigh(m - 1, 1 - par)
            product(m - 2)
        g_copy(2 * p - 2).start()
        g_copy(2 * p - 1).start()
        return 0

    lax.fori_loop(1, blocks // 2, behind, 0)
    weigh(blocks - 1, 1)
    product(blocks - 2)
    product(blocks - 1)
    g_copy(blocks - 2).start()
    g_copy(blocks - 1).start()
    pltpu.make_async_copy(g_ref, g_hbm, g_sem).wait()


def first_call(stats, mask_lines, x_rows, x_t, tab_t, tea_rows, width, tp):
    tokens, dim = x_rows.shape
    whole = pl.BlockSpec(memory_space=pltpu.VMEM)
    hbm = pl.BlockSpec(memory_space=pl.ANY)
    blocks = tokens // TOK
    return pl.pallas_call(
        functools.partial(first_kernel, tp),
        in_specs=[hbm] * 6,
        out_specs=[whole, whole, whole, hbm, whole],
        out_shape=[
            jax.ShapeDtypeStruct(stats.shape, jnp.float32),
            jax.ShapeDtypeStruct((8, 128), jnp.float32),
            jax.ShapeDtypeStruct((dim, width), jnp.float32),
            jax.ShapeDtypeStruct((tokens, width), jnp.bfloat16),
            jax.ShapeDtypeStruct((8, 128), jnp.float32),
        ],
        scratch_shapes=[
            pltpu.VMEM(stats.shape, jnp.float32),
            pltpu.VMEM(mask_lines.shape, jnp.float32),
            pltpu.VMEM((tokens, width), jnp.bfloat16),
            pltpu.VMEM((tp,) + stats.shape, jnp.float32),
            pltpu.VMEM(mask_lines.shape, jnp.float32),
            pltpu.VMEM((tokens, dim), jnp.bfloat16),
            pltpu.VMEM((dim, tokens), jnp.bfloat16),
            pltpu.VMEM((dim, width), jnp.bfloat16),
            pltpu.VMEM((tokens, width), jnp.bfloat16),
            pltpu.VMEM((TOK, width), jnp.float32),
            pltpu.VMEM((TOK, width), jnp.float32),
            pltpu.VMEM((tokens, width), jnp.float32),
            pltpu.VMEM((tokens, width), jnp.float32),
            pltpu.VMEM((tokens, 128), jnp.float32),
            pltpu.VMEM((2, TOK, 128), jnp.float32),
            pltpu.VMEM((2, TOK, 128), jnp.float32),
            pltpu.SemaphoreType.DMA((tp,)),
            pltpu.SemaphoreType.DMA((tp,)),
            pltpu.SemaphoreType.DMA,
            pltpu.SemaphoreType.DMA,
            pltpu.SemaphoreType.DMA,
            pltpu.SemaphoreType.DMA,
            pltpu.SemaphoreType.DMA((blocks,)),
            pltpu.SemaphoreType.DMA,
            pltpu.SemaphoreType.DMA,
            pltpu.SemaphoreType.DMA,
            pltpu.SemaphoreType.DMA,
        ],
        compiler_params=pltpu.CompilerParams(collective_id=0, has_side_effects=True, vmem_limit_bytes=VMEM_LIMIT),
        cost_estimate=pl.CostEstimate(flops=4 * tokens * width * dim, bytes_accessed=4 * tokens * dim, transcendentals=0),
        name="first",
    )(stats, mask_lines, x_rows, x_t, tab_t, tea_rows)


def grad_kernel(ab_ref, x_ref, xt_ref, tab_ref, tea_ref, kl_in_ref, table_ref, g_ref, kl_ref, z0_ref, z1_ref, coef_ref):
    z_refs = (z0_ref, z1_ref)
    col = z0_ref.shape[1]
    count = tab_ref.shape[1] // col
    block = pl.program_id(0)

    @pl.when(block == 0)
    def _():
        table_ref[...] = jnp.zeros_like(table_ref)
        kl_ref[...] = kl_in_ref[...]

    for k in range(2):
        for b in range(LINES):
            line = ab_ref[pl.ds(k * (ab_ref.shape[0] // 2) + block * LINES + b, 1), :]
            coef_ref[k, b * 128:(b + 1) * 128, :] = jnp.broadcast_to(line, (128, 128)).T

    def columns(n):
        return pl.ds(pl.multiple_of(n * col, col), col)

    def logits(n, par):
        z_refs[par][...] = lax.dot_general(x_ref[...], tab_ref[:, columns(n)], NN, preferred_element_type=jnp.float32)

    def weigh(n, par):
        def strip(rows, kl_acc):
            a = coef_ref[0, rows, :]
            b = coef_ref[1, rows, :]
            for q in range(col // 128):
                lanes = pl.ds(pl.multiple_of(n * col + q * 128, 128), 128)
                zq = z_refs[par][rows, q * 128:(q + 1) * 128]
                tq = tea_ref[rows, lanes].astype(jnp.float32)
                ts = jnp.tanh(zq * INV_CAP)
                tt = jnp.tanh(tq * INV_CAP)
                pa = jnp.exp2(ts * EXP_SCALE) * a
                pb = jnp.exp2(tt * EXP_SCALE) * b
                kl = pb * (tt - ts)
                for w in range(0, 64, 8):
                    kl_acc += kl[w:w + 8]
                g_ref[rows, lanes] = ((pa - pb) * (1.0 - ts * ts)).astype(jnp.bfloat16)
            return kl_acc

        if count <= 2:
            kl_ref[...] = lax.fori_loop(0, TOK // 64, lambda r, acc: strip(pl.ds(pl.multiple_of(r * 64, 64), 64), acc), kl_ref[...])
        else:
            kl_acc = kl_ref[...]
            for r in range(0, TOK, 64):
                kl_acc = strip(slice(r, r + 64), kl_acc)
            kl_ref[...] = kl_acc

    def product(n):
        table_ref[:, columns(n)] += lax.dot_general(xt_ref[...], g_ref[:, columns(n)], NN, preferred_element_type=jnp.float32)

    logits(0, 0)
    if count == 1:
        weigh(0, 0)
        product(0)
        return
    logits(1, 1)
    weigh(0, 0)

    def pair(p, _):
        for par in range(2):
            n = 2 * p + par
            logits(n, par)
            weigh(n - 1, 1 - par)
            product(n - 2)
        return 0

    if count == 4:
        pair(1, 0)
    elif count > 4:
        lax.fori_loop(1, count // 2, pair, 0)
    product(count - 2)
    weigh(count - 1, 1)
    product(count - 1)


def grad_call(ab, x_rows, x_t, tab_t, tea_rows, start, size, kl):
    tokens, dim = x_rows.shape
    col = GCOL if size % (2 * GCOL) == 0 else size
    return pl.pallas_call(
        grad_kernel,
        grid=(tokens // TOK,),
        in_specs=[
            pl.BlockSpec(ab.shape, lambda i: (0, 0)),
            pl.BlockSpec((TOK, dim), lambda i: (i, 0)),
            pl.BlockSpec((dim, TOK), lambda i: (0, i)),
            pl.BlockSpec((pl.Element(dim), pl.Element(size)), lambda i: (0, start), pipeline_mode=pl.Buffered(1)),
            pl.BlockSpec((pl.Element(TOK), pl.Element(size)), lambda i: (i * TOK, start)),
            pl.BlockSpec((8, 128), lambda i: (0, 0)),
        ],
        out_specs=[
            pl.BlockSpec((dim, size), lambda i: (0, 0)),
            pl.BlockSpec((TOK, size), lambda i: (i, 0)),
            pl.BlockSpec((8, 128), lambda i: (0, 0)),
        ],
        scratch_shapes=[
            pltpu.VMEM((TOK, col), jnp.float32),
            pltpu.VMEM((TOK, col), jnp.float32),
            pltpu.VMEM((2, TOK, 128), jnp.float32),
        ],
        out_shape=[
            jax.ShapeDtypeStruct((dim, size), jnp.float32),
            jax.ShapeDtypeStruct((tokens, size), jnp.bfloat16),
            jax.ShapeDtypeStruct((8, 128), jnp.float32),
        ],
        compiler_params=pltpu.CompilerParams(vmem_limit_bytes=VMEM_LIMIT),
        cost_estimate=pl.CostEstimate(flops=4 * tokens * size * dim, bytes_accessed=4 * tokens * size, transcendentals=0),
    )(ab, x_rows, x_t, tab_t, tea_rows, kl)


def back_kernel(half_ref, tab_ref, *refs):
    g_refs, dx_ref = refs[:-1], refs[-1]
    start = 0
    for g_ref in g_refs:
        size = g_ref.shape[1]
        step = min(size, 1024 if size % 1024 == 0 else 768)
        assert size % step == 0
        for n in range(size // step):
            cols = slice(start + n * step, start + (n + 1) * step)
            dx = lax.dot_general(tab_ref[:, cols], g_ref[:, n * step:(n + 1) * step], NT, preferred_element_type=jnp.float32)
            if start + n == 0:
                dx_ref[...] = dx
            else:
                dx_ref[...] += dx
        start += size


def back_call(tab_t, grads, half):
    dim, cols = tab_t.shape
    tokens = grads[0].shape[0]
    rows = dim // 2
    return pl.pallas_call(
        back_kernel,
        grid_spec=pltpu.PrefetchScalarGridSpec(
            num_scalar_prefetch=1,
            grid=(tokens // TOK,),
            in_specs=[pl.BlockSpec((rows, cols), lambda i, h: (h[0], 0), pipeline_mode=pl.Buffered(1))]
            + [pl.BlockSpec((TOK, g.shape[1]), lambda i, h: (i, 0)) for g in grads],
            out_specs=pl.BlockSpec((rows, TOK), lambda i, h: (0, i)),
        ),
        out_shape=jax.ShapeDtypeStruct((rows, tokens), jnp.float32),
        compiler_params=pltpu.CompilerParams(vmem_limit_bytes=VMEM_LIMIT),
        cost_estimate=pl.CostEstimate(flops=tokens * cols * dim, bytes_accessed=2 * tokens * cols, transcendentals=0),
        name="back",
    )(half[None], tab_t, *grads)


def finish_kernel(off_ref, hid_ref, gain_ref, *refs):
    piece_refs, (out_ref, sum_ref, norm_ref, a_ref, gain_buf) = refs[:-5], refs[-5:]
    dim, toks = hid_ref.shape

    @pl.when(pl.program_id(0) == 0)
    def _():
        gain_buf[...] = jnp.broadcast_to(1.0 + gain_ref[...], (128, dim)).T
        sum_ref[...] = jnp.zeros_like(sum_ref)

    hid = hid_ref[...].astype(jnp.float32)
    inv_rms = lax.rsqrt(jnp.mean(hid * hid, axis=0, keepdims=True) + NORM_EPS)
    norm_ref[...] = hid * inv_rms
    dot = jnp.zeros((1, toks), jnp.float32)
    for k, piece_ref in enumerate(piece_refs):
        rows = pl.ds(pl.multiple_of(off_ref[k], 8), piece_ref.shape[0])
        gain = gain_buf[rows, :]
        acc = sum_ref[rows, :]
        for b in range(toks // 128):
            lanes = slice(b * 128, (b + 1) * 128)
            a_ref[rows, lanes] = piece_ref[:, lanes] * gain
            acc += piece_ref[:, lanes] * norm_ref[rows, lanes]
        sum_ref[rows, :] = acc
        dot += jnp.sum(a_ref[rows, :] * norm_ref[rows, :], axis=0, keepdims=True)
    out_ref[...] = (inv_rms * (a_ref[...] - norm_ref[...] * (dot / dim))).astype(jnp.bfloat16)


def finish_call(offsets, hid_t, gain_row, pieces):
    dim, tokens = hid_t.shape
    rows = pieces[0].shape[0]
    return pl.pallas_call(
        finish_kernel,
        grid_spec=pltpu.PrefetchScalarGridSpec(
            num_scalar_prefetch=1,
            grid=(tokens // TOK,),
            in_specs=[pl.BlockSpec((dim, TOK), lambda i, o: (0, i)), pl.BlockSpec((1, dim), lambda i, o: (0, 0))]
            + [pl.BlockSpec((rows, TOK), lambda i, o: (0, i))] * len(pieces),
            out_specs=[pl.BlockSpec((dim, TOK), lambda i, o: (0, i)), pl.BlockSpec((dim, 128), lambda i, o: (0, 0))],
            scratch_shapes=[pltpu.VMEM((dim, TOK), jnp.float32), pltpu.VMEM((dim, TOK), jnp.float32), pltpu.VMEM((dim, 128), jnp.float32)],
        ),
        out_shape=[jax.ShapeDtypeStruct((dim, tokens), jnp.bfloat16), jax.ShapeDtypeStruct((dim, 128), jnp.float32)],
        compiler_params=pltpu.CompilerParams(vmem_limit_bytes=VMEM_LIMIT),
        cost_estimate=pl.CostEstimate(flops=10 * tokens * dim, bytes_accessed=8 * tokens * dim, transcendentals=0),
        name="finish",
    )(offsets, hid_t, gain_row, *pieces)


def add_kernel(own_ref, recv_ref, *refs):
    refs[-1][...] = own_ref[...] + recv_ref[...]


def add_call(own, recv, start, cols, out, after):
    dim, size = own.shape
    step = 128
    spec = pl.BlockSpec((dim, step), lambda i: (0, i))
    hold = pl.BlockSpec(memory_space=pl.ANY)
    in_specs = [spec, spec]
    operands = [own, recv]
    aliases = {}
    if out is not None:
        operands.append(out)
        aliases = {2: 0}
    operands += after
    in_specs += [hold] * (len(operands) - 2)
    return pl.pallas_call(
        add_kernel,
        grid=(size // step,),
        in_specs=in_specs,
        out_specs=pl.BlockSpec((dim, step), lambda i: (0, start // step + i)),
        out_shape=jax.ShapeDtypeStruct((dim, cols), jnp.float32),
        input_output_aliases=aliases,
        cost_estimate=pl.CostEstimate(flops=size * dim, bytes_accessed=12 * size * dim, transcendentals=0),
    )(*operands)


def exchange_partner(i, step):
    if step == 0:
        return i ^ 1
    return i ^ (2 if (i & 1) == (step - 1) else 4)


def place(bits, rows):
    return (bits[0] * (rows // 2) + bits[1] * (rows // 4) + bits[2] * (rows // 8)).astype(jnp.int32)


def solution(mesh):
    tp = mesh.shape["tp"]

    def local_step(hid_rows, w_final, tab_rows, tea_rows, mask_rows):
        tokens, dim = hid_rows.shape
        hid_t, tab_t = hid_rows.T, tab_rows.T
        mask_lines = mask_rows.reshape(tokens // 128, 128)
        x_rows, x_t, stats = stats_call(mask_lines, w_final.reshape(1, dim), hid_t, tab_t, tea_rows)

        swap = [(0, 1), (1, 0)]
        start = 0
        parts, grads = [], []
        for c, size in enumerate(CHUNKS):
            if c == 0:
                ab, log_part, table_c, g, kl = first_call(stats, mask_lines, x_rows, x_t, tab_t, tea_rows, size, tp)
            else:
                table_c, g, kl = grad_call(ab, x_rows, x_t, tab_t, tea_rows, start, size, kl)
            grads.append(g)
            recv = lax.ppermute(table_c, "dp", swap)
            parts.append((start, table_c, recv))
            start += size

        me = lax.axis_index("tp")
        core, xb, yb = me & 1, (me >> 1) & 1, (me >> 2) & 1
        bits = (core, jnp.where(core == 0, xb, yb), jnp.where(core == 0, yb, xb))
        perms = [[(i, exchange_partner(i, s)) for i in range(tp)] for s in range(3)]
        away = back_call(tab_t, grads, 1 - core)
        recv = lax.ppermute(away, "tp", perms[0])
        keep = back_call(tab_t, grads, core)
        for s in (1, 2):
            half = keep.shape[0] // 2
            gone = (1 - bits[s]) * half
            away = lax.dynamic_slice_in_dim(keep, gone, half, 0) + lax.dynamic_slice_in_dim(recv, gone, half, 0)
            away = lax.ppermute(away, "tp", perms[s])
            kept = bits[s] * half
            keep = lax.dynamic_slice_in_dim(keep, kept, half, 0) + lax.dynamic_slice_in_dim(recv, kept, half, 0)
            recv = away
        own = keep + recv
        pieces = [own]
        for s in (2, 1, 0):
            pieces += [lax.ppermute(piece, "tp", perms[s]) for piece in pieces]
        c, u, v = bits
        spots = [(c, u, v), (c, u, 1 - v), (c, 1 - u, v), (c, 1 - u, 1 - v)]
        spots += [(1 - c, v, u), (1 - c, v, 1 - u), (1 - c, 1 - v, u), (1 - c, 1 - v, 1 - u)]
        offsets = jnp.stack([place(spot, dim) for spot in spots])

        loss_part = lax.psum(SOFT_CAP * jnp.sum(kl), "tp") + jnp.sum(log_part)
        grad_h, gain_part = finish_call(offsets, hid_t, w_final.reshape(1, dim), pieces)
        small = jnp.concatenate([jnp.sum(gain_part, axis=1), jnp.full((1024 - dim,), loss_part)])
        other = lax.ppermute(small, "dp", swap)
        small = small + other

        out = None
        for n, (begin, own, recv) in enumerate(parts):
            last = n == len(parts) - 1
            out = add_call(own, recv, begin, tab_t.shape[1], out, [grad_h, small] if last else [])
        return small[dim], grad_h.T, small[:dim], out.T

    return jax.shard_map(local_step, mesh=mesh, in_specs=(P('dp', None), P(None), P('tp', None), P('dp', 'tp'), P('dp')), out_specs=(P(), P('dp', None), P(None), P('tp', None)), check_vma=False)
```

```python
import functools

import jax
import jax.numpy as jnp
from jax import lax
from jax.experimental import pallas as pl
from jax.experimental.pallas import tpu as pltpu
from jax.sharding import PartitionSpec as P


SOFT_CAP = 30.0
NORM_EPS = 1e-6
INV_CAP = 1.0 / SOFT_CAP
EXP_SCALE = SOFT_CAP * 1.4426950408889634
TOK = 512
LINES = TOK // 128
RUN = 16
STOK = 256
COL = 512
GCOL = 256
CHUNKS = ((256,), (256,), (512,), (1024,), (2048,), (1536, 384, 128))
VMEM_LIMIT = 62 * 1024 * 1024
MESH = pl.DeviceIdType.MESH
NT = (((1,), (1,)), ((), ()))
NN = (((1,), (0,)), ((), ()))


def stats_kernel(mask_hbm, gain_hbm, hid_hbm, tab_hbm, tea_hbm, x_hbm, xt_hbm, out_ref, gain_buf,
                 mask_buf, hid_buf, x_buf, xt_buf, tab_buf, tea_buf, rows_ref, z0_ref, z1_ref, acc_ref, sum_ref, flag_buf, row_buf,
                 flags, order, hid_sem, tab_sem, tea_sem, flag_sem, row_sem, out_sem):
    z_refs = (z0_ref, z1_ref)
    dim, tokens = hid_hbm.shape
    count = tab_hbm.shape[1] // COL
    slabs = tokens // TOK
    runs = tokens // RUN
    per = STOK // RUN

    def hid_copy(i):
        cols = pl.ds(i * TOK, TOK)
        return pltpu.make_async_copy(hid_hbm.at[:, cols], hid_buf.at[:, cols], hid_sem.at[i])

    def tab_copy(i):
        cols = pl.ds(i * COL, COL)
        return pltpu.make_async_copy(tab_hbm.at[:, cols], tab_buf.at[:, cols], tab_sem)

    mask_copy = pltpu.make_async_copy(mask_hbm, mask_buf, flag_sem)
    row_copy = pltpu.make_async_copy(gain_hbm, row_buf, row_sem)
    mask_copy.start()
    row_copy.start()
    for i in range(slabs):
        hid_copy(i).start()
    for i in range(count):
        tab_copy(i).start()

    mask_copy.wait()
    flag = mask_buf[...]
    for shift in (1, 2, 4, 8):
        flag = jnp.maximum(flag, pltpu.roll(flag, 128 - shift, 1))
    flag_buf[...] = (flag > 0).astype(jnp.int32)
    flag_copy = pltpu.make_async_copy(flag_buf, flags, flag_sem)
    flag_copy.start()
    row_copy.wait()
    gain_buf[...] = jnp.broadcast_to(1.0 + row_buf[...], (128, dim)).T
    sum_ref[...] = jnp.ones_like(sum_ref)
    flag_copy.wait()

    def tea_start(b):
        slot = lax.rem(b, 2)

        def one(k, _):
            src = pl.ds(pl.multiple_of(order[b * per + k] * RUN, RUN), RUN)
            dst = pl.ds(pl.multiple_of(k * RUN, RUN), RUN)
            pltpu.make_async_copy(tea_hbm.at[src, :], tea_buf.at[slot, dst, :], tea_sem.at[slot]).start()
            return 0

        lax.fori_loop(0, per, one, 0)

    def tea_wait(b):
        slot = lax.rem(b, 2)
        pltpu.make_async_copy(tea_hbm.at[pl.ds(0, STOK), :], tea_buf.at[slot], tea_sem.at[slot]).wait()

    def slab(i, found, marks):
        pltpu.make_async_copy(hid_hbm.at[:, pl.ds(0, TOK)], hid_buf.at[:, pl.ds(0, TOK)], hid_sem.at[i]).wait()
        for r in range(marks):
            run = i * marks + r
            order[found] = run
            found = found + flags[lax.div(i * marks, 128 // RUN) + r // (128 // RUN), r % (128 // RUN) * RUN]
        for b in range(LINES):
            lanes = pl.ds(pl.multiple_of(i * TOK + b * 128, 128), 128)
            hid = hid_buf[:, lanes].astype(jnp.float32)
            inv_rms = lax.rsqrt(jnp.mean(hid * hid, axis=0, keepdims=True) + NORM_EPS)
            xb = (hid * inv_rms * gain_buf[...]).astype(jnp.bfloat16)
            xt_buf[:, lanes] = xb
            x_buf[lanes, :] = xb.T
        return found

    early = slabs // 2
    found = lax.fori_loop(0, early, lambda i, found: slab(i, found, runs // early), 0)
    last = order[jnp.maximum(found - 1, 0)]
    last = jnp.where(found > 0, last, 0)
    for k in range(2 * per):
        order[found + k] = last
    blocks = lax.div(found + per - 1, per)

    @pl.when(blocks > 0)
    def _():
        tea_start(0)

    lax.fori_loop(early, slabs, lambda i, _: slab(i, 0, 0), 0)
    x_out = pltpu.make_async_copy(x_buf, x_hbm, out_sem.at[0])
    xt_out = pltpu.make_async_copy(xt_buf, xt_hbm, out_sem.at[1])
    x_out.start()
    xt_out.start()
    pltpu.make_async_copy(tab_hbm, tab_buf, tab_sem).wait()

    def gather(b):
        slot = lax.rem(b, 2)
        for k in range(per):
            src = pl.ds(pl.multiple_of(order[b * per + k] * RUN, RUN), RUN)
            rows_ref[slot, k * RUN:(k + 1) * RUN, :] = x_buf[src, :]

    def logits(b, n, par):
        cols = slice(n * COL, (n + 1) * COL)
        z_refs[par][...] = lax.dot_general(rows_ref[lax.rem(b, 2)], tab_buf[:, cols], NN, preferred_element_type=jnp.float32)

    def collect(b, n, par):
        slot = lax.rem(b, 2)
        for r in range(0, STOK, 64):
            rows = slice(r, r + 64)
            acc_s = jnp.zeros((64, 128), jnp.float32) if n == 0 else acc_ref[0, rows, :]
            acc_t = jnp.zeros((64, 128), jnp.float32) if n == 0 else acc_ref[1, rows, :]
            for q in range(COL // 128):
                zq = z_refs[par][rows, q * 128:(q + 1) * 128]
                tq = tea_buf[slot, rows, n * COL + q * 128:n * COL + (q + 1) * 128].astype(jnp.float32)
                acc_s += jnp.exp2(jnp.tanh(zq * INV_CAP) * EXP_SCALE)
                acc_t += jnp.exp2(jnp.tanh(tq * INV_CAP) * EXP_SCALE)
            acc_ref[0, rows, :] = acc_s
            acc_ref[1, rows, :] = acc_t

    @pl.when(blocks > 0)
    def _():
        gather(0)
        logits(0, 0, 0)

    def block(b, _):
        @pl.when(b + 1 < blocks)
        def _():
            tea_start(b + 1)

        tea_wait(b)
        for n in range(count):
            if n + 1 < count:
                logits(b, n + 1, (n + 1) % 2)
            else:
                gather(b + 1)
                logits(b + 1, 0, 0)
            collect(b, n, n % 2)
        for k in range(per):
            dst = pl.ds(pl.multiple_of(order[b * per + k] * RUN, RUN), RUN)
            for s in range(2):
                sum_ref[s, dst, :] = acc_ref[s, k * RUN:(k + 1) * RUN, :]
        return 0

    lax.fori_loop(0, blocks, block, 0)

    def lines(i, _):
        for s in range(2):
            for b in range(8):
                rows = pl.ds(pl.multiple_of((i * 8 + b) * 128, 128), 128)
                out_ref[s * (tokens // 128) + i * 8 + b, :] = jnp.sum(sum_ref[s, rows, :].T, axis=0)
        return 0

    lax.fori_loop(0, tokens // 1024, lines, 0)
    x_out.wait()
    xt_out.wait()


def stats_call(mask_lines, gain_row, hid_t, tab_t, tea_rows):
    dim, tokens = hid_t.shape
    cols = tab_t.shape[1]
    assert (cols // COL) % 2 == 0
    hbm = pl.BlockSpec(memory_space=pl.ANY)
    vmem = pl.BlockSpec(memory_space=pltpu.VMEM)
    per = STOK // RUN
    return pl.pallas_call(
        stats_kernel,
        in_specs=[hbm] * 5,
        out_specs=[hbm, hbm, vmem, vmem],
        out_shape=[
            jax.ShapeDtypeStruct((tokens, dim), jnp.bfloat16),
            jax.ShapeDtypeStruct((dim, tokens), jnp.bfloat16),
            jax.ShapeDtypeStruct((tokens // 64, 128), jnp.float32),
            jax.ShapeDtypeStruct((dim, 128), jnp.float32),
        ],
        scratch_shapes=[
            pltpu.VMEM(mask_lines.shape, jnp.float32),
            pltpu.VMEM((dim, tokens), jnp.bfloat16),
            pltpu.VMEM((tokens, dim), jnp.bfloat16),
            pltpu.VMEM((dim, tokens), jnp.bfloat16),
            pltpu.VMEM((dim, cols), jnp.bfloat16),
            pltpu.VMEM((2, STOK, cols), jnp.bfloat16),
            pltpu.VMEM((2, STOK, dim), jnp.bfloat16),
            pltpu.VMEM((STOK, COL), jnp.float32),
            pltpu.VMEM((STOK, COL), jnp.float32),
            pltpu.VMEM((2, STOK, 128), jnp.float32),
            pltpu.VMEM((2, tokens, 128), jnp.float32),
            pltpu.VMEM((tokens // 128, 128), jnp.int32),
            pltpu.VMEM((1, dim), jnp.float32),
            pltpu.SMEM((tokens // 128, 128), jnp.int32),
            pltpu.SMEM((tokens // RUN + 2 * per,), jnp.int32),
            pltpu.SemaphoreType.DMA((tokens // TOK,)),
            pltpu.SemaphoreType.DMA,
            pltpu.SemaphoreType.DMA((2,)),
            pltpu.SemaphoreType.DMA,
            pltpu.SemaphoreType.DMA,
            pltpu.SemaphoreType.DMA((2,)),
        ],
        compiler_params=pltpu.CompilerParams(vmem_limit_bytes=VMEM_LIMIT),
        cost_estimate=pl.CostEstimate(flops=2 * tokens * cols * dim, bytes_accessed=2 * tokens * cols, transcendentals=0),
        name="stats",
    )(mask_lines, gain_row, hid_t, tab_t, tea_rows)


def first_kernel(tp, stats_hbm, mask_hbm, x_hbm, xt_hbm, tab_hbm, tea_hbm, ab_ref, log_ref, table_ref, g_hbm, kl_ref,
                 stats_ref, mask_ref, g_ref, slots, mask_slot, x_buf, xt_buf, tab_buf, tea_buf, z0_ref, z1_ref, stu_ref, tea_ref, gap_ref, coef0_ref, coef1_ref,
                 send_sem, recv_sem, msend_sem, mrecv_sem, stats_sem, mask_sem, x_sem, xt_sem, tab_sem, tea_sem, g_sem):
    dp_me = lax.axis_index("dp")
    me = lax.axis_index("tp")
    tokens, width = g_ref.shape
    blocks = tokens // TOK

    def g_copy(m):
        rows = pl.ds(pl.multiple_of(m * TOK, TOK), TOK)
        return pltpu.make_async_copy(g_ref.at[rows, :], g_hbm.at[rows, :], g_sem)

    def x_copy(m):
        rows = pl.ds(m * TOK, TOK)
        return pltpu.make_async_copy(x_hbm.at[rows, :], x_buf.at[rows, :], x_sem.at[m])

    tab_copy = pltpu.make_async_copy(tab_hbm.at[:, pl.ds(0, width)], tab_buf, tab_sem)
    tea_copy = pltpu.make_async_copy(tea_hbm.at[:, pl.ds(0, width)], tea_buf, tea_sem)
    xt_copy = pltpu.make_async_copy(xt_hbm, xt_buf, xt_sem)
    stats_copy = pltpu.make_async_copy(stats_hbm, stats_ref, stats_sem)
    mask_copy = pltpu.make_async_copy(mask_hbm, mask_ref, mask_sem)
    barrier = pltpu.get_barrier_semaphore()
    for d in range(1, tp):
        pl.semaphore_signal(barrier, inc=1, device_id=(dp_me, lax.rem(me + d, tp)), device_id_type=MESH)
    pl.semaphore_signal(barrier, inc=1, device_id=(1 - dp_me, me), device_id_type=MESH)
    stats_copy.start()
    mask_copy.start()
    tab_copy.start()
    x_copy(0).start()
    tea_copy.start()
    for m in range(1, blocks):
        x_copy(m).start()
    xt_copy.start()

    z_refs = (z0_ref, z1_ref)

    def logits(m, par):
        rows = pl.ds(pl.multiple_of(m * TOK, TOK), TOK)
        z_refs[par][...] = lax.dot_general(x_buf[rows, :], tab_buf[...], NN, preferred_element_type=jnp.float32)

    def terms(m, par):
        for r in range(0, TOK, 64):
            rows = pl.ds(pl.multiple_of(m * TOK + r, 64), 64)
            gap = jnp.zeros((64, 128), jnp.float32)
            for q in range(width // 128):
                lanes = slice(q * 128, (q + 1) * 128)
                ts = jnp.tanh(z_refs[par][r:r + 64, lanes] * INV_CAP)
                tt = jnp.tanh(tea_buf[rows, lanes].astype(jnp.float32) * INV_CAP)
                slope = 1.0 - ts * ts
                eb = jnp.exp2(tt * EXP_SCALE)
                stu_ref[rows, lanes] = jnp.exp2(ts * EXP_SCALE) * slope
                tea_ref[rows, lanes] = eb * slope
                gap += eb * (tt - ts)
            gap_ref[rows, :] = gap

    stats_copy.wait()
    mask_copy.wait()
    pl.semaphore_wait(barrier, tp)
    copies = []
    for d in range(1, tp):
        copies.append(pltpu.make_async_remote_copy(
            src_ref=stats_ref, dst_ref=slots.at[me], send_sem=send_sem.at[d], recv_sem=recv_sem.at[d],
            device_id=(dp_me, lax.rem(me + d, tp)), device_id_type=MESH))
    copies.append(pltpu.make_async_remote_copy(
        src_ref=mask_ref, dst_ref=mask_slot, send_sem=msend_sem, recv_sem=mrecv_sem,
        device_id=(1 - dp_me, me), device_id_type=MESH))
    for copy in copies:
        copy.start()
    slots[me] = stats_ref[...]
    tab_copy.wait()
    x_copy(0).wait()
    tea_copy.wait()
    logits(0, 0)

    def ahead(p, _):
        for par in range(2):
            m = 2 * p + par
            pltpu.make_async_copy(x_hbm.at[pl.ds(0, TOK), :], x_buf.at[pl.ds(0, TOK), :], x_sem.at[m + 1]).wait()
            logits(m + 1, 1 - par)
            terms(m, par)
        return 0

    if blocks > 2:
        lax.fori_loop(0, blocks // 2 - 1, ahead, 0)
    x_copy(blocks - 1).wait()
    logits(blocks - 1, 1)
    terms(blocks - 2, 0)
    terms(blocks - 1, 1)

    xt_copy.wait()
    for copy in copies:
        copy.wait()
    total = slots[0]
    for k in range(1, tp):
        total += slots[k]
    mask = mask_ref[...]
    weight = mask / (jnp.sum(mask, keepdims=True) + jnp.sum(mask_slot[...], keepdims=True))
    half = mask.shape[0]
    ab_ref[:half, :] = weight / total[:half]
    ab_ref[half:, :] = weight / total[half:]
    logs = weight * (jnp.log(total[:half]) - jnp.log(total[half:]))
    log_ref[...] = logs

    kl_ref[...] = jnp.zeros_like(kl_ref)
    table_ref[...] = jnp.zeros_like(table_ref)
    coef_refs = (coef0_ref, coef1_ref)

    def spread(m, par):
        for k in range(2):
            for b in range(LINES):
                line = ab_ref[pl.ds(k * half + m * LINES + b, 1), :]
                coef_refs[par][k, b * 128:(b + 1) * 128, :] = jnp.broadcast_to(line, (128, 128)).T

    def weigh(m, par):
        kl_acc = kl_ref[:8, :]
        for r in range(0, TOK, 64):
            rows = pl.ds(pl.multiple_of(m * TOK + r, 64), 64)
            a = coef_refs[par][0, r:r + 64, :]
            b = coef_refs[par][1, r:r + 64, :]
            gap = gap_ref[rows, :] * b
            for w in range(0, 64, 8):
                kl_acc += gap[w:w + 8]
            for q in range(width // 128):
                lanes = slice(q * 128, (q + 1) * 128)
                g_ref[rows, lanes] = (stu_ref[rows, lanes] * a - tea_ref[rows, lanes] * b).astype(jnp.bfloat16)
        kl_ref[:8, :] = kl_acc

    def product(m):
        rows = pl.ds(pl.multiple_of(m * TOK, TOK), TOK)
        table_ref[...] += lax.dot_general(xt_buf[:, rows], g_ref[rows, :], NN, preferred_element_type=jnp.float32)

    spread(0, 0)
    spread(1, 1)
    weigh(0, 0)

    def behind(p, _):
        for par in range(2):
            m = 2 * p + par
            spread(m, par)
            weigh(m - 1, 1 - par)
            product(m - 2)
        g_copy(2 * p - 2).start()
        g_copy(2 * p - 1).start()
        return 0

    lax.fori_loop(1, blocks // 2, behind, 0)
    weigh(blocks - 1, 1)
    product(blocks - 2)
    product(blocks - 1)
    g_copy(blocks - 2).start()
    g_copy(blocks - 1).start()
    pltpu.make_async_copy(g_ref, g_hbm, g_sem).wait()


def first_call(stats, mask_lines, x_rows, x_t, tab_t, tea_rows, width, tp):
    tokens, dim = x_rows.shape
    whole = pl.BlockSpec(memory_space=pltpu.VMEM)
    hbm = pl.BlockSpec(memory_space=pl.ANY)
    blocks = tokens // TOK
    return pl.pallas_call(
        functools.partial(first_kernel, tp),
        in_specs=[hbm] * 6,
        out_specs=[whole, whole, whole, hbm, whole],
        out_shape=[
            jax.ShapeDtypeStruct(stats.shape, jnp.float32),
            jax.ShapeDtypeStruct(mask_lines.shape, jnp.float32),
            jax.ShapeDtypeStruct((dim, width), jnp.float32),
            jax.ShapeDtypeStruct((tokens, width), jnp.bfloat16),
            jax.ShapeDtypeStruct((32, 128), jnp.float32),
        ],
        scratch_shapes=[
            pltpu.VMEM(stats.shape, jnp.float32),
            pltpu.VMEM(mask_lines.shape, jnp.float32),
            pltpu.VMEM((tokens, width), jnp.bfloat16),
            pltpu.VMEM((tp,) + stats.shape, jnp.float32),
            pltpu.VMEM(mask_lines.shape, jnp.float32),
            pltpu.VMEM((tokens, dim), jnp.bfloat16),
            pltpu.VMEM((dim, tokens), jnp.bfloat16),
            pltpu.VMEM((dim, width), jnp.bfloat16),
            pltpu.VMEM((tokens, width), jnp.bfloat16),
            pltpu.VMEM((TOK, width), jnp.float32),
            pltpu.VMEM((TOK, width), jnp.float32),
            pltpu.VMEM((tokens, width), jnp.float32),
            pltpu.VMEM((tokens, width), jnp.float32),
            pltpu.VMEM((tokens, 128), jnp.float32),
            pltpu.VMEM((2, TOK, 128), jnp.float32),
            pltpu.VMEM((2, TOK, 128), jnp.float32),
            pltpu.SemaphoreType.DMA((tp,)),
            pltpu.SemaphoreType.DMA((tp,)),
            pltpu.SemaphoreType.DMA,
            pltpu.SemaphoreType.DMA,
            pltpu.SemaphoreType.DMA,
            pltpu.SemaphoreType.DMA,
            pltpu.SemaphoreType.DMA((blocks,)),
            pltpu.SemaphoreType.DMA,
            pltpu.SemaphoreType.DMA,
            pltpu.SemaphoreType.DMA,
            pltpu.SemaphoreType.DMA,
        ],
        compiler_params=pltpu.CompilerParams(collective_id=0, has_side_effects=True, vmem_limit_bytes=VMEM_LIMIT),
        cost_estimate=pl.CostEstimate(flops=4 * tokens * width * dim, bytes_accessed=4 * tokens * dim, transcendentals=0),
        name="first",
    )(stats, mask_lines, x_rows, x_t, tab_t, tea_rows)


def grad_kernel(pieces, ab_ref, x_ref, xt_ref, tab_ref, tea_ref, kl_in_ref, *refs):
    out_refs = refs[:pieces]
    g_ref, kl_ref, z0_ref, z1_ref, coef_ref = refs[pieces:pieces + 5]
    table_ref = refs[-1] if pieces > 1 else out_refs[0]
    z_refs = (z0_ref, z1_ref)
    col = z0_ref.shape[1]
    count = tab_ref.shape[1] // col
    block = pl.program_id(0)

    @pl.when(block == 0)
    def _():
        table_ref[...] = jnp.zeros_like(table_ref)
        kl_ref[...] = kl_in_ref[...]

    for k in range(2):
        for b in range(LINES):
            line = ab_ref[pl.ds(k * (ab_ref.shape[0] // 2) + block * LINES + b, 1), :]
            coef_ref[k, b * 128:(b + 1) * 128, :] = jnp.broadcast_to(line, (128, 128)).T

    def columns(n):
        return pl.ds(pl.multiple_of(n * col, col), col)

    def logits(n, par):
        z_refs[par][...] = lax.dot_general(x_ref[...], tab_ref[:, columns(n)], NN, preferred_element_type=jnp.float32)

    def weigh(n, par):
        kl_acc = kl_ref[:8, :]
        for r in range(0, TOK, 64):
            rows = slice(r, r + 64)
            a = coef_ref[0, rows, :]
            b = coef_ref[1, rows, :]
            for q in range(col // 128):
                lanes = pl.ds(pl.multiple_of(n * col + q * 128, 128), 128)
                zq = z_refs[par][rows, q * 128:(q + 1) * 128]
                tq = tea_ref[rows, lanes].astype(jnp.float32)
                ts = jnp.tanh(zq * INV_CAP)
                tt = jnp.tanh(tq * INV_CAP)
                pa = jnp.exp2(ts * EXP_SCALE) * a
                pb = jnp.exp2(tt * EXP_SCALE) * b
                kl = pb * (tt - ts)
                for w in range(0, 64, 8):
                    kl_acc += kl[w:w + 8]
                g_ref[rows, lanes] = ((pa - pb) * (1.0 - ts * ts)).astype(jnp.bfloat16)
        kl_ref[:8, :] = kl_acc

    def product(n):
        table_ref[:, columns(n)] += lax.dot_general(xt_ref[...], g_ref[:, columns(n)], NN, preferred_element_type=jnp.float32)

    logits(0, 0)
    if count == 1:
        weigh(0, 0)
        product(0)
        return
    logits(1, 1)
    weigh(0, 0)

    def pair(p, _):
        for par in range(2):
            n = 2 * p + par
            logits(n, par)
            weigh(n - 1, 1 - par)
            product(n - 2)
        return 0

    if count == 4:
        pair(1, 0)
    elif count > 4:
        lax.fori_loop(1, count // 2, pair, 0)
    product(count - 2)
    weigh(count - 1, 1)
    product(count - 1)
    if pieces > 1:
        @pl.when(block == pl.num_programs(0) - 1)
        def _():
            begin = 0
            for out_ref in out_refs:
                out_ref[...] = table_ref[:, begin:begin + out_ref.shape[1]]
                begin += out_ref.shape[1]


def grad_call(ab, x_rows, x_t, tab_t, tea_rows, start, pieces, kl):
    tokens, dim = x_rows.shape
    size = sum(pieces)
    col = GCOL if size % (2 * GCOL) == 0 else size
    split = len(pieces) > 1
    return pl.pallas_call(
        functools.partial(grad_kernel, len(pieces)),
        grid=(tokens // TOK,),
        in_specs=[
            pl.BlockSpec(ab.shape, lambda i: (0, 0)),
            pl.BlockSpec((TOK, dim), lambda i: (i, 0)),
            pl.BlockSpec((dim, TOK), lambda i: (0, i)),
            pl.BlockSpec((pl.Element(dim), pl.Element(size)), lambda i: (0, start), pipeline_mode=pl.Buffered(1)),
            pl.BlockSpec((pl.Element(TOK), pl.Element(size)), lambda i: (i * TOK, start)),
            pl.BlockSpec((32, 128), lambda i: (0, 0)),
        ],
        out_specs=[pl.BlockSpec((dim, width), lambda i: (0, 0)) for width in pieces] + [
            pl.BlockSpec((TOK, size), lambda i: (i, 0)),
            pl.BlockSpec((32, 128), lambda i: (0, 0)),
        ],
        scratch_shapes=[
            pltpu.VMEM((TOK, col), jnp.float32),
            pltpu.VMEM((TOK, col), jnp.float32),
            pltpu.VMEM((2, TOK, 128), jnp.float32),
        ] + [pltpu.VMEM((dim, size), jnp.float32)] * split,
        out_shape=[jax.ShapeDtypeStruct((dim, width), jnp.float32) for width in pieces] + [
            jax.ShapeDtypeStruct((tokens, size), jnp.bfloat16),
            jax.ShapeDtypeStruct((32, 128), jnp.float32),
        ],
        compiler_params=pltpu.CompilerParams(vmem_limit_bytes=VMEM_LIMIT),
        cost_estimate=pl.CostEstimate(flops=4 * tokens * size * dim, bytes_accessed=4 * tokens * size, transcendentals=0),
    )(ab, x_rows, x_t, tab_t, tea_rows, kl)


def back_kernel(half_ref, tab_ref, *refs):
    g_refs, dx_ref = refs[:-1], refs[-1]
    start = 0
    for g_ref in g_refs:
        size = g_ref.shape[1]
        step = min(size, 1024 if size % 1024 == 0 else 768)
        assert size % step == 0
        for n in range(size // step):
            cols = slice(start + n * step, start + (n + 1) * step)
            dx = lax.dot_general(tab_ref[:, cols], g_ref[:, n * step:(n + 1) * step], NT, preferred_element_type=jnp.float32)
            if start + n == 0:
                dx_ref[...] = dx
            else:
                dx_ref[...] += dx
        start += size


def back_call(tab_t, grads, half):
    dim, cols = tab_t.shape
    tokens = grads[0].shape[0]
    rows = dim // 2
    return pl.pallas_call(
        back_kernel,
        grid_spec=pltpu.PrefetchScalarGridSpec(
            num_scalar_prefetch=1,
            grid=(tokens // TOK,),
            in_specs=[pl.BlockSpec((rows, cols), lambda i, h: (h[0], 0), pipeline_mode=pl.Buffered(1))]
            + [pl.BlockSpec((TOK, g.shape[1]), lambda i, h: (i, 0)) for g in grads],
            out_specs=pl.BlockSpec((rows, TOK), lambda i, h: (0, i)),
        ),
        out_shape=jax.ShapeDtypeStruct((rows, tokens), jnp.float32),
        compiler_params=pltpu.CompilerParams(vmem_limit_bytes=VMEM_LIMIT),
        cost_estimate=pl.CostEstimate(flops=tokens * cols * dim, bytes_accessed=2 * tokens * cols, transcendentals=0),
        name="back",
    )(half[None], tab_t, *grads)


def finish_kernel(off_ref, hid_ref, gain_ref, *refs):
    piece_refs, (out_ref, sum_ref, norm_ref, a_ref) = refs[:-4], refs[-4:]
    dim, toks = hid_ref.shape

    @pl.when(pl.program_id(0) == 0)
    def _():
        sum_ref[...] = jnp.zeros_like(sum_ref)

    hid = hid_ref[...].astype(jnp.float32)
    inv_rms = lax.rsqrt(jnp.mean(hid * hid, axis=0, keepdims=True) + NORM_EPS)
    norm_ref[...] = hid * inv_rms
    dot = jnp.zeros((1, toks), jnp.float32)
    for k, piece_ref in enumerate(piece_refs):
        rows = pl.ds(pl.multiple_of(off_ref[k], 8), piece_ref.shape[0])
        gain = gain_ref[rows, :]
        acc = sum_ref[rows, :]
        for b in range(toks // 128):
            lanes = slice(b * 128, (b + 1) * 128)
            a_ref[rows, lanes] = piece_ref[:, lanes] * gain
            acc += piece_ref[:, lanes] * norm_ref[rows, lanes]
        sum_ref[rows, :] = acc
        dot += jnp.sum(a_ref[rows, :] * norm_ref[rows, :], axis=0, keepdims=True)
    out_ref[...] = (inv_rms * (a_ref[...] - norm_ref[...] * (dot / dim))).astype(jnp.bfloat16)


def finish_call(offsets, hid_t, gain_cols, pieces):
    dim, tokens = hid_t.shape
    rows = pieces[0].shape[0]
    return pl.pallas_call(
        finish_kernel,
        grid_spec=pltpu.PrefetchScalarGridSpec(
            num_scalar_prefetch=1,
            grid=(tokens // TOK,),
            in_specs=[pl.BlockSpec((dim, TOK), lambda i, o: (0, i)), pl.BlockSpec((dim, 128), lambda i, o: (0, 0))]
            + [pl.BlockSpec((rows, TOK), lambda i, o: (0, i))] * len(pieces),
            out_specs=[pl.BlockSpec((dim, TOK), lambda i, o: (0, i)), pl.BlockSpec((dim, 128), lambda i, o: (0, 0))],
            scratch_shapes=[pltpu.VMEM((dim, TOK), jnp.float32), pltpu.VMEM((dim, TOK), jnp.float32)],
        ),
        out_shape=[jax.ShapeDtypeStruct((dim, tokens), jnp.bfloat16), jax.ShapeDtypeStruct((dim, 128), jnp.float32)],
        compiler_params=pltpu.CompilerParams(vmem_limit_bytes=VMEM_LIMIT),
        cost_estimate=pl.CostEstimate(flops=10 * tokens * dim, bytes_accessed=8 * tokens * dim, transcendentals=0),
        name="finish",
    )(offsets, hid_t, gain_cols, *pieces)


def add_kernel(own_ref, recv_ref, *refs):
    refs[-1][...] = own_ref[...] + recv_ref[...]


def add_call(own, recv, start, cols, out, after):
    dim, size = own.shape
    step = 128
    spec = pl.BlockSpec((dim, step), lambda i: (0, i))
    hold = pl.BlockSpec(memory_space=pl.ANY)
    in_specs = [spec, spec]
    operands = [own, recv]
    aliases = {}
    if out is not None:
        operands.append(out)
        aliases = {2: 0}
    operands += after
    in_specs += [hold] * (len(operands) - 2)
    return pl.pallas_call(
        add_kernel,
        grid=(size // step,),
        in_specs=in_specs,
        out_specs=pl.BlockSpec((dim, step), lambda i: (0, start // step + i)),
        out_shape=jax.ShapeDtypeStruct((dim, cols), jnp.float32),
        input_output_aliases=aliases,
        cost_estimate=pl.CostEstimate(flops=size * dim, bytes_accessed=12 * size * dim, transcendentals=0),
    )(*operands)


def exchange_partner(i, step):
    if step == 0:
        return i ^ 1
    return i ^ (2 if (i & 1) == (step - 1) else 4)


def place(bits, rows):
    return (bits[0] * (rows // 2) + bits[1] * (rows // 4) + bits[2] * (rows // 8)).astype(jnp.int32)


def solution(mesh):
    tp = mesh.shape["tp"]

    def local_step(hid_rows, w_final, tab_rows, tea_rows, mask_rows):
        tokens, dim = hid_rows.shape
        hid_t, tab_t = hid_rows.T, tab_rows.T
        mask_lines = mask_rows.reshape(tokens // 128, 128)
        x_rows, x_t, stats, gain_cols = stats_call(mask_lines, w_final.reshape(1, dim), hid_t, tab_t, tea_rows)

        swap = [(0, 1), (1, 0)]
        start = 0
        parts, grads = [], []
        for c, pieces in enumerate(CHUNKS):
            if c == 0:
                ab, log_part, *tables, g, kl = first_call(stats, mask_lines, x_rows, x_t, tab_t, tea_rows, sum(pieces), tp)
            else:
                *tables, g, kl = grad_call(ab, x_rows, x_t, tab_t, tea_rows, start, pieces, kl)
            grads.append(g)
            for table in tables:
                recv = lax.ppermute(table, "dp", swap)
                parts.append((start, table, recv))
                start += table.shape[1]

        me = lax.axis_index("tp")
        core, xb, yb = me & 1, (me >> 1) & 1, (me >> 2) & 1
        bits = (core, jnp.where(core == 0, xb, yb), jnp.where(core == 0, yb, xb))
        perms = [[(i, exchange_partner(i, s)) for i in range(tp)] for s in range(3)]
        away = back_call(tab_t, grads, 1 - core)
        recv = lax.ppermute(away, "tp", perms[0])
        keep = back_call(tab_t, grads, core)
        for s in (1, 2):
            half = keep.shape[0] // 2
            gone = (1 - bits[s]) * half
            away = lax.dynamic_slice_in_dim(keep, gone, half, 0) + lax.dynamic_slice_in_dim(recv, gone, half, 0)
            away, keep, recv = lax.optimization_barrier((away, keep, recv))
            away = lax.ppermute(away, "tp", perms[s])
            kept = bits[s] * half
            keep = lax.dynamic_slice_in_dim(keep, kept, half, 0) + lax.dynamic_slice_in_dim(recv, kept, half, 0)
            keep, kl = lax.optimization_barrier((keep, kl))
            recv = away
        own = keep + recv
        pieces = [own]
        for s in (2, 1, 0):
            pieces += [lax.ppermute(piece, "tp", perms[s]) for piece in pieces]
        c, u, v = bits
        spots = [(c, u, v), (c, u, 1 - v), (c, 1 - u, v), (c, 1 - u, 1 - v)]
        spots += [(1 - c, v, u), (1 - c, v, 1 - u), (1 - c, 1 - v, u), (1 - c, 1 - v, 1 - u)]
        offsets = jnp.stack([place(spot, dim) for spot in spots])

        loss_part = lax.psum(SOFT_CAP * jnp.sum(kl), "tp") + jnp.sum(log_part)
        grad_h, gain_part = finish_call(offsets, hid_t, gain_cols, pieces)
        small = jnp.concatenate([jnp.sum(gain_part, axis=1), jnp.full((1024 - dim,), loss_part)])
        other = lax.ppermute(small, "dp", swap)
        small = small + other

        out = None
        for n, (begin, own, recv) in enumerate(parts):
            last = n == len(parts) - 1
            out = add_call(own, recv, begin, tab_t.shape[1], out, [grad_h, small] if last else [])
        return small[dim], grad_h.T, small[:dim], out.T

    return jax.shard_map(local_step, mesh=mesh, in_specs=(P('dp', None), P(None), P('tp', None), P('dp', 'tp'), P('dp')), out_specs=(P(), P('dp', None), P(None), P('tp', None)), check_vma=False)
```
